128 devices in a mesh: gx: 4 (over z), gy: 4 (over y), gz: 8 (over x, core).
Axes of the slice: x: 4, y: 4, z: 4, core: 2. Of those that a mesh axis runs over, the one named last changes fastest.
Arguments:
- fields: float32 [40, 32, 64, 1024], P(None, 'gx', 'gy', 'gz'), may hold values from 0.1 to 1.5
- source: float32 [40, 32, 64, 1024], P(None, 'gx', 'gy', 'gz'), may hold values from 0.005 to 0.2
- velocity: float32 [3, 32, 64, 1024], P(None, 'gx', 'gy', 'gz'), may hold values from -1 to 1
- diffusivity: float32 [40], replicated, may hold values from 0.02 to 0.09
- reacting: int32 [32, 64, 8], P('gx', 'gy', 'gz'), may hold values from 0 to 1, as said below
- counts: int32 [32, 64, 8], P('gx', 'gy', 'gz'), may hold values from 1 to 4
- mechanism: int32 [4, 100], replicated, may hold values from 0 to 21
- prefactor: float32 [100], replicated, may hold values from 0.5 to 5
- activation: float32 [100], replicated, may hold values from 0.3 to 3
- heat_release: float32 [100], replicated, may hold values from 0.01 to 0.1
Outputs:
- evolved: float32 [40, 32, 64, 1024], P(None, 'gx', 'gy', 'gz')
The draws below stay inside these ranges and needn't reach their ends.
Inputs may be any that keep to these rules, and one draw needn't show every extreme that they name: `reacting`: over all devices exactly 2048 blocks react, and on one device all of its 128 blocks react.
All inputs are finite; a program needn't handle non-finite values.
Results may differ from the reference program's by a relative error of at most 0.0003.
Values sent between devices are 32-bit elements; how exact they have to be, the bound alone decides.
No kernel may reach another device: no remote copies, remote signals or barrier semaphores. Data moves between devices by JAX's collectives and lax.ppermute only.
A program may use at most 128 MiB of HBM per device.

```python
import math
import jax
import jax.numpy as jnp
from jax import lax

FIELDS = 40
SPECIES = 22
REACTIONS = 100
CZ = 128
SUB = 4
CX = 8
CY = 16
NX = 32
NY = 64
NZ = 1024
CAP = 16
N_GZ = 8


def draw_reacting(key, part):
    along_x = NX // CX
    along_y = NY // CY
    layers = NZ // CZ
    devices = along_x * along_y * layers
    all_blocks = NX * NY * layers
    key_level, key_top, key_jitter = jax.random.split(key, 3)
    x_index = lax.broadcasted_iota(jnp.int32, (NX, NY, layers), 0)
    y_index = lax.broadcasted_iota(jnp.int32, (NX, NY, layers), 1)
    z_index = lax.broadcasted_iota(jnp.int32, (NX, NY, layers), 2)
    owners = x_index // CX * (along_y * layers) + y_index // CY * layers + z_index
    levels = jax.random.randint(key_level, (devices,), 0, 4)
    busiest = jax.random.randint(key_top, (), 0, devices)
    levels = jnp.where(jnp.arange(devices, dtype=jnp.int32) == busiest, 16, levels)
    jitter = jax.random.randint(key_jitter, (NX, NY, layers), 0, 1024)
    scores = (jnp.take(levels, owners) * 256 + jitter).reshape(-1) * all_blocks + jnp.arange(all_blocks, dtype=jnp.int32)
    wanted = CAP * devices
    ranking = jnp.argsort(-scores)
    placed = jnp.zeros((all_blocks,), jnp.int32).at[ranking].set(jnp.arange(all_blocks, dtype=jnp.int32))
    return (placed < wanted).astype(jnp.int32).reshape(NX, NY, layers)


def plant(values, rng, low, high):
    dims = values.shape
    spot = [jax.random.randint(jax.random.fold_in(rng, axis), (), 0, dims[axis]) for axis in range(len(dims))]
    values = values.at[tuple(spot)].set(low)
    longest = dims.index(max(dims))
    spot[longest] = (spot[longest] + 1) % dims[longest]
    return values.at[tuple(spot)].set(high)


def level_of(rng, extent, shards, low, high):
    loudness = 1.0
    for position, shards_of in shards:
        steps = jax.random.uniform(jax.random.fold_in(jax.random.fold_in(rng, 6), position), (shards_of,), jnp.float32, low / len(shards), high / len(shards))
        loudness = loudness * jnp.repeat(jnp.exp(steps), extent[position] // shards_of).reshape((-1,) + (1,) * (len(extent) - 1 - position))
    return loudness


def setup_inputs(seed: int = 0) -> dict:
    key_of = jax.random.split(jax.random.key(seed), 11)
    return {
        "fields": jnp.clip(jnp.exp(math.log(1.5) - 2.7080502 * jax.random.uniform(key_of[0], (FIELDS, NX, NY, NZ), jnp.float32) ** level_of(key_of[0], (FIELDS, NX, NY, NZ), ((1, 4), (2, 4), (3, 8)), -0.2, 0.2)), 0.1, 1.5),
        "source": jnp.clip(jnp.exp(math.log(0.2) - 3.6888795 * jax.random.uniform(key_of[1], (FIELDS, NX, NY, NZ), jnp.float32) ** level_of(key_of[1], (FIELDS, NX, NY, NZ), ((1, 4), (2, 4), (3, 8)), -0.2, 0.2)), 0.005, 0.2),
        "velocity": jnp.clip(jax.random.uniform(key_of[2], (3, NX, NY, NZ), jnp.float32, -1.0, 1.0) * level_of(key_of[2], (3, NX, NY, NZ), ((1, 4), (2, 4), (3, 8)), -0.4, 0.0), -1.0, 1.0),
        "diffusivity": jnp.clip(jnp.exp(jax.random.uniform(key_of[3], (FIELDS,), jnp.float32, math.log(0.02), math.log(0.09))), 0.02, 0.09),
        "reacting": draw_reacting(jax.random.fold_in(key_of[10], 71), 0),
        "counts": plant(jax.random.randint(key_of[5], (NX, NY, N_GZ), 1, SUB + 1), jax.random.fold_in(key_of[5], 1), 1, SUB).astype(jnp.int32),
        "mechanism": plant(jax.random.randint(key_of[6], (4, REACTIONS), 0, SPECIES), jax.random.fold_in(key_of[6], 1), 0, SPECIES - 1).astype(jnp.int32),
        "prefactor": jnp.clip(jnp.exp(jax.random.uniform(key_of[7], (REACTIONS,), jnp.float32, math.log(0.5), math.log(5.0))), 0.5, 5.0),
        "activation": jnp.clip(jnp.exp(jax.random.uniform(key_of[8], (REACTIONS,), jnp.float32, math.log(0.3), math.log(3.0))), 0.3, 3.0),
        "heat_release": jnp.clip(jnp.exp(jax.random.uniform(key_of[9], (REACTIONS,), jnp.float32, math.log(0.01), math.log(0.1))), 0.01, 0.1),
    }


courant = 0.15
chem_step = 0.25


def advance(fields, velocity, diffusivity, source):
    padded = jnp.pad(fields, ((0, 0), (1, 1), (1, 1), (1, 1)))
    up_cells = (padded[:, 2:, 1:-1, 1:-1], padded[:, 1:-1, 2:, 1:-1], padded[:, 1:-1, 1:-1, 2:])
    down_cells = (padded[:, :-2, 1:-1, 1:-1], padded[:, 1:-1, :-2, 1:-1], padded[:, 1:-1, 1:-1, :-2])
    diffuse = diffusivity[:, None, None, None]
    result = fields + source
    for direction in range(3):
        flow_speed = velocity[direction][None]
        result = result - courant * (jnp.maximum(flow_speed, 0.0) * (fields - down_cells[direction]) + jnp.minimum(flow_speed, 0.0) * (up_cells[direction] - fields))
        result = result + diffuse * (up_cells[direction] + down_cells[direction] - 2.0 * fields)
    return result


def react(chem_state, sub_counts, mechanism, prefactor, activation, heat_release):
    species_row = lax.broadcasted_iota(jnp.int32, (1, SPECIES), 1)
    species_col = lax.broadcasted_iota(jnp.int32, (SPECIES, 1), 0)
    reactant_ids = mechanism[0:2].reshape(-1).astype(jnp.int32)
    takers = (reactant_ids[:, None] == species_row).astype(jnp.float32)
    losers = jnp.transpose(takers)
    makers = (mechanism[2][None, :] == species_col).astype(jnp.float32) + (mechanism[3][None, :] == species_col).astype(jnp.float32)
    makers = jnp.concatenate([makers, heat_release[None, :].astype(jnp.float32)], 0)
    interval = chem_step / sub_counts.astype(jnp.float32)
    for substep in range(SUB):
        fractions = chem_state[:SPECIES]
        temper = chem_state[SPECIES]
        rate_const = prefactor[:, None, None] * jnp.exp(-activation[:, None, None] / temper[None])
        paired = jnp.take(fractions, reactant_ids, axis=0)
        reactant_one = paired[:REACTIONS]
        reactant_two = paired[REACTIONS:]
        progress = rate_const * reactant_one * reactant_two
        loss_rate = jnp.einsum("kj,jnc->knc", losers, jnp.concatenate([rate_const * reactant_two, rate_const * reactant_one], 0), precision=lax.Precision.HIGHEST)
        gain_rate = jnp.einsum("kj,jnc->knc", makers, progress, precision=lax.Precision.HIGHEST)
        widths = interval[None, :, None]
        renewed_fractions = (fractions + widths * gain_rate[:SPECIES]) / (1.0 + widths * loss_rate)
        renewed_temper = temper + interval[:, None] * gain_rate[SPECIES]
        renewed = jnp.concatenate([renewed_fractions, renewed_temper[None]], 0)
        chem_state = jnp.where((substep < sub_counts)[None, :, None], renewed, chem_state)
    return chem_state


def reference(fields, source, velocity, diffusivity, reacting, counts, mechanism, prefactor, activation, heat_release):
    current = fields
    for substep in range(2):
        current = advance(current, velocity, diffusivity, source)
    blocks = current.reshape(FIELDS, NX, NY * N_GZ, CZ)
    chemistry = jnp.moveaxis(blocks[:SPECIES + 1], 1, 0)
    marked_rows = reacting.reshape(NX, NY * N_GZ)
    count_rows = counts.reshape(NX, NY * N_GZ)

    def one_row(items):
        chem_state, marked, sub_counts = items
        reacted_row = react(chem_state, sub_counts, mechanism, prefactor, activation, heat_release)
        return jnp.where((marked == 1)[None, :, None], reacted_row, chem_state)

    reacted = lax.map(one_row, (chemistry, marked_rows, count_rows))
    merged = jnp.concatenate([jnp.moveaxis(reacted, 0, 1), blocks[SPECIES + 1:]], 0)
    return merged.reshape(FIELDS, NX, NY, NZ)
```

```python
import functools

import jax
import jax.numpy as jnp
from jax import lax
from jax.experimental import pallas as pl
from jax.experimental.pallas import tpu as pltpu
from jax.sharding import PartitionSpec as P

FIELDS = 40
SPECIES = 22
REACTIONS = 100
SUB = 4
CX = 8
CY = 16
CZ = 128
ROWS = CX * CY
GROUP = 8
STEPS = FIELDS // GROUP
BATCH = 8
COURANT = 0.15
CHEM_STEP = 0.25
LOG2E = 1.4426950408889634
AXES = ("gx", "gy", "gz")


def place(axis):
    index = lax.axis_index(axis)
    even = lax.rem(index, 2) == 0
    return even, index > 0, index < lax.axis_size(axis) - 1


def swapped(value, axis, start):
    size = lax.axis_size(axis)
    pairs = []
    for low in range(start, size, 2):
        high = (low + 1) % size
        pairs += [(low, high), (high, low)]
    return lax.ppermute(value, axis, pairs)


def pick_faces(step, block, sends, columns, turned):
    xs0, xs1, ys0, ys1, zs0, zs1 = sends
    xeven, _, _ = place("gx")
    yeven, _, _ = place("gy")
    zeven, _, _ = place("gz")
    high_x = pl.multiple_of(jnp.where(xeven, (CX - 1) * CY, 0), CY)
    low_x = pl.multiple_of(jnp.where(xeven, 0, (CX - 1) * CY), CY)
    high_y = jnp.where(yeven, CY - 1, 0)
    low_y = jnp.where(yeven, 0, CY - 1)
    for f in range(GROUP):
        xs0[f] = block[f, pl.ds(high_x, CY), :]
        xs1[f] = block[f, pl.ds(low_x, CY), :]
        ys0[f] = block[f, pl.ds(high_y, CX, stride=CY), :]
        ys1[f] = block[f, pl.ds(low_y, CX, stride=CY), :]
    lane = lax.broadcasted_iota(jnp.int32, (8, CZ), 1)
    first = step * (2 * GROUP)
    for r in range(0, ROWS, 8):
        total = columns[r : r + 8, :]
        for f in range(GROUP):
            moved = pltpu.roll(block[f, r : r + 8, :], first + 2 * f + 1, 1)
            here = lane - first
            total = jnp.where((here >= 2 * f) & (here < 2 * f + 2), moved, total)
        columns[r : r + 8, :] = total

    @pl.when(step == STEPS - 1)
    def _():
        turned[...] = columns[...].T
        highs = turned[pl.ds(0, FIELDS, stride=2), :]
        lows = turned[pl.ds(1, FIELDS, stride=2), :]
        zs0[...] = jnp.where(zeven, highs, lows)
        zs1[...] = jnp.where(zeven, lows, highs)


def faces_kernel(fields, xs0, xs1, ys0, ys1, zs0, zs1, columns, turned):
    step = pl.program_id(0)

    @pl.when(step == 0)
    def _():
        columns[...] = jnp.zeros_like(columns)

    pick_faces(step, fields, (xs0, xs1, ys0, ys1, zs0, zs1), columns, turned)


def set_up(velocity, halos, weights, columns, turned):
    zh0, zh1 = halos
    for r in range(0, ROWS, 8):
        rest = jnp.ones((8, CZ), jnp.float32)
        for a in range(3):
            speed = velocity[a, r : r + 8, :]
            below = COURANT * jnp.maximum(speed, 0.0)
            above = -COURANT * jnp.minimum(speed, 0.0)
            weights[2 * a, r : r + 8, :] = below
            weights[2 * a + 1, r : r + 8, :] = above
            rest = rest - (below + above)
        weights[6, r : r + 8, :] = rest
    zeven, has_low, has_high = place("gz")
    columns[...] = jnp.zeros_like(columns)
    first, second = zh0[...], zh1[...]
    high = jnp.where(has_high, jnp.where(zeven, first, second), 0.0)
    low = jnp.where(has_low, jnp.where(zeven, second, first), 0.0)
    columns[pl.ds(0, FIELDS, stride=2), :] = high
    columns[pl.ds(1, FIELDS, stride=2), :] = low
    turned[...] = columns[...].T


def move_group(step, block, source, halos, diffusivity, weights, turned, result, base):
    xh0, xh1, yh0, yh1 = halos
    xeven, x_low, x_high = place("gx")
    yeven, y_low, y_high = place("gy")
    row = lax.broadcasted_iota(jnp.int32, (CY, CZ), 0)
    lane = lax.broadcasted_iota(jnp.int32, (CY, CZ), 1)
    diffuse = [diffusivity[step * GROUP + f] for f in range(GROUP)]
    for x in range(CX):
        here = slice(x * CY, (x + 1) * CY)
        share = [weights[k, here, :] for k in range(7)]
        edge = turned[here, :]
        for f in range(GROUP):
            cell = block[f, here, :]
            if x > 0:
                xm = block[f, (x - 1) * CY : x * CY, :]
            else:
                xm = jnp.where(x_low, jnp.where(xeven, xh1[f], xh0[f]), 0.0)
            if x < CX - 1:
                xp = block[f, (x + 1) * CY : (x + 2) * CY, :]
            else:
                xp = jnp.where(x_high, jnp.where(xeven, xh0[f], xh1[f]), 0.0)
            y0 = yh0[f, x : x + 1, :]
            y1 = yh1[f, x : x + 1, :]
            y_below = jnp.where(y_low, jnp.where(yeven, y1, y0), 0.0)
            y_above = jnp.where(y_high, jnp.where(yeven, y0, y1), 0.0)
            ym = jnp.where(row == 0, y_below, pltpu.roll(cell, 1, 0))
            yp = jnp.where(row == CY - 1, y_above, pltpu.roll(cell, CY - 1, 0))
            halo = pltpu.roll(edge, CZ - 1 - 2 * f - step * (2 * GROUP), 1)
            zm = jnp.where(lane == 0, halo, pltpu.roll(cell, 1, 1))
            zp = jnp.where(lane == CZ - 1, halo, pltpu.roll(cell, CZ - 1, 1))
            around = (xm + xp) + (ym + yp) + (zm + zp)
            carried = (
                (share[0] * xm + share[1] * xp)
                + (share[2] * ym + share[3] * yp)
                + (share[4] * zm + share[5] * zp)
            )
            kept = cell * (share[6] - 6.0 * diffuse[f])
            result[base + f, here, :] = (kept + source[f, here, :]) + (
                carried + diffuse[f] * around
            )


def first_kernel(
    diffusivity, fields, source, velocity, xh0, xh1, yh0, yh1, zh0, zh1,
    moved, xs0, xs1, ys0, ys1, zs0, zs1, weights, columns, turned, faces, across,
):
    step = pl.program_id(0)

    @pl.when(step == 0)
    def _():
        set_up(velocity, (zh0, zh1), weights, columns, turned)
        faces[...] = jnp.zeros_like(faces)

    move_group(
        step, fields, source, (xh0, xh1, yh0, yh1), diffusivity, weights, turned, moved, 0
    )
    pick_faces(step, moved, (xs0, xs1, ys0, ys1, zs0, zs1), faces, across)


def react(state, counts, mechanism, prefactor, activation, heat_release, sums):
    taken_a, taken_b, made_c, made_d = sums
    for s in range(SPECIES):
        for part in sums:
            part[s] = jnp.zeros((ROWS, CZ), jnp.float32)

    def substep(number, carry):
        for base in range(0, ROWS, 8 * BATCH):
            rows = [slice(base + 8 * v, base + 8 * v + 8) for v in range(BATCH)]
            cold = [-LOG2E / state[SPECIES, r, :] for r in rows]

            def reaction(j, heats):
                a, b = mechanism[0, j], mechanism[1, j]
                c, d = mechanism[2, j], mechanism[3, j]
                strength, barrier, heat = prefactor[j], activation[j], heat_release[j]
                rates = []
                for v in range(BATCH):
                    rate = strength * jnp.exp2(barrier * cold[v])
                    rates.append(rate * (state[a, rows[v], :] * state[b, rows[v], :]))
                for part, index in ((taken_a, a), (taken_b, b), (made_c, c), (made_d, d)):
                    old = [part[index, rows[v], :] for v in range(BATCH)]
                    for v in range(BATCH):
                        part[index, rows[v], :] = old[v] + rates[v]
                return tuple(heats[v] + heat * rates[v] for v in range(BATCH))

            nothing = tuple(jnp.zeros((8, CZ), jnp.float32) for _ in range(BATCH))
            heats = lax.fori_loop(0, REACTIONS, reaction, nothing, unroll=2)

            for v in range(BATCH):
                many = counts[rows[v], :]
                live = many > number.astype(jnp.float32)
                width = CHEM_STEP / jnp.maximum(many, 1.0)
                old = state[SPECIES, rows[v], :]
                state[SPECIES, rows[v], :] = jnp.where(live, old + width * heats[v], old)

            def species(s, carry):
                empty = jnp.zeros((8, CZ), jnp.float32)
                for v in range(BATCH):
                    many = counts[rows[v], :]
                    live = many > number.astype(jnp.float32)
                    width = CHEM_STEP / jnp.maximum(many, 1.0)
                    old = state[s, rows[v], :]
                    lost = width * (taken_a[s, rows[v], :] + taken_b[s, rows[v], :])
                    gained = width * (made_c[s, rows[v], :] + made_d[s, rows[v], :])
                    new = old * ((old + gained) / (old + lost))
                    state[s, rows[v], :] = jnp.where(live, new, old)
                    for part in sums:
                        part[s, rows[v], :] = empty
                return carry

            lax.fori_loop(0, SPECIES, species, 0)
        return carry

    lax.fori_loop(0, SUB, substep, 0)


def second_kernel(
    diffusivity, mechanism, prefactor, activation, heat_release,
    fields, source, velocity, counts, xh0, xh1, yh0, yh1, zh0, zh1,
    out, weights, columns, turned, state, sum_a, sum_b, sum_c, sum_d, sems,
):
    step = pl.program_id(0)

    def leaving(group):
        part = pl.ds(group * GROUP, GROUP)
        return pltpu.make_async_copy(state.at[part], out.at[part], sems.at[group])

    @pl.when(step == 0)
    def _():
        set_up(velocity, (zh0, zh1), weights, columns, turned)

    move_group(
        step, fields, source, (xh0, xh1, yh0, yh1), diffusivity, weights, turned, state,
        step * GROUP,
    )

    @pl.when(step == STEPS - 1)
    def _():
        for group in range(3, STEPS):
            leaving(group).start()
        react(
            state, counts, mechanism, prefactor, activation, heat_release,
            (sum_a, sum_b, sum_c, sum_d),
        )
        for group in range(3):
            leaving(group).start()
        for group in range(STEPS):
            leaving(group).wait()


def group_spec(*tail):
    return pl.BlockSpec((GROUP,) + tail, lambda g: (g,) + (0,) * len(tail))


def whole_spec(*shape):
    return pl.BlockSpec(shape, lambda g: (0,) * len(shape))


SCALARS = pl.BlockSpec(memory_space=pltpu.SMEM)
HALO_SPECS = [
    group_spec(CY, CZ), group_spec(CY, CZ), group_spec(CX, CZ), group_spec(CX, CZ),
    whole_spec(FIELDS, CZ), whole_spec(FIELDS, CZ),
]
HALO_SHAPES = [
    jax.ShapeDtypeStruct(shape, jnp.float32)
    for shape in (
        (FIELDS, CY, CZ), (FIELDS, CY, CZ), (FIELDS, CX, CZ), (FIELDS, CX, CZ),
        (FIELDS, CZ), (FIELDS, CZ),
    )
]
SQUARE = pltpu.VMEM((ROWS, CZ), jnp.float32)
WEIGHTS = pltpu.VMEM((7, ROWS, CZ), jnp.float32)
PARAMS = pltpu.CompilerParams(dimension_semantics=("arbitrary",))


def exchanged(sends):
    got = []
    for k, axis in enumerate(AXES):
        got += [swapped(sends[2 * k], axis, 0), swapped(sends[2 * k + 1], axis, 1)]
    return got


def body(
    fields, source, velocity, diffusivity, reacting, counts, mechanism, prefactor, activation,
    heat_release,
):
    fields = fields.reshape(FIELDS, ROWS, CZ)
    source = source.reshape(FIELDS, ROWS, CZ)
    velocity = velocity.reshape(3, ROWS, CZ)
    many = jnp.where(reacting == 1, counts, 0).astype(jnp.float32)
    many = jnp.broadcast_to(many, (CX, CY, CZ)).reshape(ROWS, CZ)

    sends = pl.pallas_call(
        faces_kernel,
        grid=(STEPS,),
        in_specs=[group_spec(ROWS, CZ)],
        out_specs=HALO_SPECS,
        out_shape=HALO_SHAPES,
        scratch_shapes=[SQUARE, SQUARE],
        compiler_params=PARAMS,
        name="faces",
    )(fields)
    halos = exchanged(sends)
    moved, *sends = pl.pallas_call(
        first_kernel,
        grid=(STEPS,),
        in_specs=[SCALARS, group_spec(ROWS, CZ), group_spec(ROWS, CZ), whole_spec(3, ROWS, CZ)]
        + HALO_SPECS,
        out_specs=[group_spec(ROWS, CZ)] + HALO_SPECS,
        out_shape=[jax.ShapeDtypeStruct((FIELDS, ROWS, CZ), jnp.float32)] + HALO_SHAPES,
        scratch_shapes=[WEIGHTS, SQUARE, SQUARE, SQUARE, SQUARE],
        compiler_params=PARAMS,
        name="first",
    )(diffusivity, fields, source, velocity, *halos)
    halos = exchanged(sends)
    sums = [pltpu.VMEM((SPECIES, ROWS, CZ), jnp.float32)] * 4
    out = pl.pallas_call(
        second_kernel,
        grid=(STEPS,),
        in_specs=[SCALARS] * 5
        + [group_spec(ROWS, CZ), group_spec(ROWS, CZ), whole_spec(3, ROWS, CZ)]
        + [whole_spec(ROWS, CZ)]
        + HALO_SPECS,
        out_specs=pl.BlockSpec(memory_space=pl.ANY),
        out_shape=jax.ShapeDtypeStruct((FIELDS, ROWS, CZ), jnp.float32),
        scratch_shapes=[WEIGHTS, SQUARE, SQUARE, pltpu.VMEM((FIELDS, ROWS, CZ), jnp.float32)]
        + sums
        + [pltpu.SemaphoreType.DMA((STEPS,))],
        compiler_params=PARAMS,
        name="second",
    )(
        diffusivity, mechanism, prefactor, activation, heat_release,
        moved, source, velocity, many, *halos,
    )
    return out.reshape(FIELDS, CX, CY, CZ)


def solution(mesh):
    grid = P(None, "gx", "gy", "gz")
    placed = (
        grid, grid, grid, P(), P("gx", "gy", "gz"), P("gx", "gy", "gz"), P(), P(), P(), P(),
    )
    return jax.shard_map(body, mesh=mesh, in_specs=placed, out_specs=grid, check_vma=False)
```

```python
import jax
import jax.numpy as jnp
from jax import lax
from jax.experimental import pallas as pl
from jax.experimental.pallas import tpu as pltpu
from jax.sharding import PartitionSpec as P

FIELDS = 40
SPECIES = 22
REACTIONS = 100
SUB = 4
CX = 8
CY = 16
CZ = 128
ROWS = CX * CY
GROUP = 8
STEPS = FIELDS // GROUP
BATCH = 16
UNROLL = 2
COURANT = 0.15
CHEM_STEP = 0.25
LOG2E = 1.4426950408889634
AXES = ("gx", "gy", "gz")


def place(axis):
    index = lax.axis_index(axis)
    even = lax.rem(index, 2) == 0
    return even, index > 0, index < lax.axis_size(axis) - 1


def swapped(value, axis, start):
    size = lax.axis_size(axis)
    pairs = []
    for low in range(start, size, 2):
        high = (low + 1) % size
        pairs += [(low, high), (high, low)]
    return lax.ppermute(value, axis, pairs)


def x_rows():
    xeven, _, _ = place("gx")
    high = pl.multiple_of(jnp.where(xeven, (CX - 1) * CY, 0), CY)
    low = pl.multiple_of(jnp.where(xeven, 0, (CX - 1) * CY), CY)
    return high, low


def pick_x(block, sends):
    xs0, xs1 = sends
    high, low = x_rows()
    for f in range(GROUP):
        xs0[f] = block[f, pl.ds(high, CY), :]
        xs1[f] = block[f, pl.ds(low, CY), :]


def pick_yz(step, block, sends, columns):
    ys0, ys1 = sends
    yeven, _, _ = place("gy")
    high_y = jnp.where(yeven, CY - 1, 0)
    low_y = jnp.where(yeven, 0, CY - 1)
    for f in range(GROUP):
        ys0[f] = block[f, pl.ds(high_y, CX, stride=CY), :]
        ys1[f] = block[f, pl.ds(low_y, CX, stride=CY), :]
    lane = lax.broadcasted_iota(jnp.int32, (8, CZ), 1)
    first = step * (2 * GROUP)
    for r in range(0, ROWS, 8):
        total = columns[r : r + 8, :]
        for f in range(GROUP):
            moved = pltpu.roll(block[f, r : r + 8, :], first + 2 * f + 1, 1)
            here = lane - first
            total = jnp.where((here >= 2 * f) & (here < 2 * f + 2), moved, total)
        columns[r : r + 8, :] = total


def turn_faces(zs0, zs1, columns, turned):
    zeven, _, _ = place("gz")
    turned[...] = columns[...].T
    highs = turned[pl.ds(0, FIELDS, stride=2), :]
    lows = turned[pl.ds(1, FIELDS, stride=2), :]
    zs0[...] = jnp.where(zeven, highs, lows)
    zs1[...] = jnp.where(zeven, lows, highs)


def group_of(refs, step):
    return [ref.at[pl.ds(step * GROUP, GROUP)] for ref in refs]


def faces_kernel(
    fields, source, velocity, held, kept, weights, xs0, xs1, ys0, ys1, zs0, zs1,
    speeds, columns, turned, sems,
):
    def arriving(whole, local, step, k):
        part = pl.ds(step * GROUP, GROUP)
        return pltpu.make_async_copy(whole.at[part], local.at[part], sems.at[k + step])

    for step in range(STEPS):
        arriving(fields, held, step, 0).start()
    fetch = pltpu.make_async_copy(velocity, speeds, sems.at[2 * STEPS])
    fetch.start()
    for step in range(STEPS):
        arriving(source, kept, step, STEPS).start()
    columns[...] = jnp.zeros_like(columns)

    @pl.loop(0, STEPS)
    def _(step):
        arriving(fields, held, step, 0).wait()
        block, *sends = group_of((held, xs0, xs1, ys0, ys1), step)
        pick_x(block, sends[:2])
        pick_yz(step, block, sends[2:], columns)

    turn_faces(zs0, zs1, columns, turned)
    fetch.wait()
    set_up(speeds, weights)
    for step in range(STEPS):
        arriving(source, kept, step, STEPS).wait()


def set_up(velocity, weights):
    for r in range(0, ROWS, 8):
        rest = jnp.ones((8, CZ), jnp.float32)
        for a in range(3):
            speed = velocity[a, r : r + 8, :]
            below = COURANT * jnp.maximum(speed, 0.0)
            above = -COURANT * jnp.minimum(speed, 0.0)
            weights[2 * a, r : r + 8, :] = below
            weights[2 * a + 1, r : r + 8, :] = above
            rest = rest - (below + above)
        weights[6, r : r + 8, :] = rest


def move_group(step, block, source, diffusivity, weights, result):
    row = lax.broadcasted_iota(jnp.int32, (CY, CZ), 0)
    lane = lax.broadcasted_iota(jnp.int32, (CY, CZ), 1)
    diffuse = [diffusivity[step * GROUP + f] for f in range(GROUP)]
    for x in range(CX):
        here = slice(x * CY, (x + 1) * CY)
        share = [weights[k, here, :] for k in range(7)]
        for f in range(GROUP):
            cell = block[f, here, :]
            ym = jnp.where(row == 0, 0.0, pltpu.roll(cell, 1, 0))
            yp = jnp.where(row == CY - 1, 0.0, pltpu.roll(cell, CY - 1, 0))
            zm = jnp.where(lane == 0, 0.0, pltpu.roll(cell, 1, 1))
            zp = jnp.where(lane == CZ - 1, 0.0, pltpu.roll(cell, CZ - 1, 1))
            around = (ym + yp) + (zm + zp)
            carried = (share[2] * ym + share[3] * yp) + (share[4] * zm + share[5] * zp)
            if x > 0:
                xm = block[f, (x - 1) * CY : x * CY, :]
                around, carried = around + xm, carried + share[0] * xm
            if x < CX - 1:
                xp = block[f, (x + 1) * CY : (x + 2) * CY, :]
                around, carried = around + xp, carried + share[1] * xp
            kept = cell * (share[6] - 6.0 * diffuse[f])
            result[f, here, :] = (kept + source[f, here, :]) + (carried + diffuse[f] * around)


def turn_halos(zh0, zh1, columns, turned):
    zeven, has_low, has_high = place("gz")
    columns[...] = jnp.zeros_like(columns)
    first, second = zh0[...], zh1[...]
    high = jnp.where(has_high, jnp.where(zeven, first, second), 0.0)
    low = jnp.where(has_low, jnp.where(zeven, second, first), 0.0)
    columns[pl.ds(0, FIELDS, stride=2), :] = high
    columns[pl.ds(1, FIELDS, stride=2), :] = low
    turned[...] = columns[...].T


def close_group(step, partial, halos, diffusivity, weights, turned, y_edges, result):
    xh0, xh1, yh0, yh1 = halos
    y_lows, y_highs = y_edges
    xeven, x_low, x_high = place("gx")
    yeven, y_low, y_high = place("gy")
    row = lax.broadcasted_iota(jnp.int32, (8, CZ), 0)
    lane = lax.broadcasted_iota(jnp.int32, (8, CZ), 1)
    one_low = jnp.where(row == 0, 1.0, 0.0)
    one_high = jnp.where(row == 7, 1.0, 0.0)
    one_z = jnp.where((lane == 0) | (lane == CZ - 1), 1.0, 0.0)
    diffuse = [diffusivity[step * GROUP + f] for f in range(GROUP)]
    for f in range(GROUP):
        first, second = yh0[f], yh1[f]
        y_lows[f] = jnp.where(y_low, jnp.where(yeven, second, first), 0.0)
        y_highs[f] = jnp.where(y_high, jnp.where(yeven, first, second), 0.0)
    for x in range(CX):
        for half in range(2):
            here = slice(x * CY + 8 * half, x * CY + 8 * half + 8)
            part = slice(8 * half, 8 * half + 8)
            edge = turned[here, :]
            share_y = weights[2 + half, here, :] * (one_high if half else one_low)
            share_z = jnp.where(
                lane == 0,
                weights[4, here, :],
                jnp.where(lane == CZ - 1, weights[5, here, :], 0.0),
            )
            for f in range(GROUP):
                y_near = (y_highs if half else y_lows)[f, x : x + 1, :]
                z_near = pltpu.roll(edge, CZ - 1 - 2 * f - step * (2 * GROUP), 1)
                one_y = one_high if half else one_low
                more = (share_y + diffuse[f] * one_y) * y_near
                more = more + (share_z + diffuse[f] * one_z) * z_near
                if x == 0:
                    near = jnp.where(xeven, xh1[f, part, :], xh0[f, part, :])
                    near = jnp.where(x_low, near, 0.0)
                    more = more + (weights[0, here, :] + diffuse[f]) * near
                if x == CX - 1:
                    near = jnp.where(xeven, xh0[f, part, :], xh1[f, part, :])
                    near = jnp.where(x_high, near, 0.0)
                    more = more + (weights[1, here, :] + diffuse[f]) * near
                result[f, here, :] = partial[f, here, :] + more


def first_edge_kernel(
    diffusivity, partial, weights, xh0, xh1, yh0, yh1, zh0, zh1,
    moved, xs0, xs1, ys0, ys1, zs0, zs1, columns, turned, faces, across, y_lows, y_highs,
):
    turn_halos(zh0, zh1, columns, turned)
    faces[...] = jnp.zeros_like(faces)

    @pl.loop(0, STEPS)
    def _(step):
        block, *halos = group_of((partial, xh0, xh1, yh0, yh1), step)
        (result,) = group_of((moved,), step)
        close_group(
            step, block, halos, diffusivity, weights, turned, (y_lows, y_highs), result
        )

    @pl.loop(0, STEPS)
    def _(step):
        result, *sends = group_of((moved, xs0, xs1, ys0, ys1), step)
        pick_x(result, sends[:2])
        pick_yz(step, result, sends[2:], faces)

    turn_faces(zs0, zs1, faces, across)


def inner_kernel(diffusivity, fields, source, weights, partial):
    @pl.loop(0, STEPS)
    def _(step):
        block, more, result = group_of((fields, source, partial), step)
        move_group(step, block, more, diffusivity, weights, result)


def react(state, counts, mechanism, prefactor, activation, heat_release, sums):
    taken_a, taken_b, made_c, made_d = sums
    for part in sums:
        part[...] = jnp.zeros_like(part)

    def substep(number, carry):
        for base in range(0, ROWS, 8 * BATCH):
            rows = [slice(base + 8 * v, base + 8 * v + 8) for v in range(BATCH)]
            cold = [-LOG2E / state[SPECIES, r, :] for r in rows]

            def reaction(j, heats):
                a, b = mechanism[0, j], mechanism[1, j]
                c, d = mechanism[2, j], mechanism[3, j]
                strength, barrier, heat = prefactor[j], activation[j], heat_release[j]
                rates = []
                for v in range(BATCH):
                    rate = strength * jnp.exp2(barrier * cold[v])
                    rates.append(rate * (state[a, rows[v], :] * state[b, rows[v], :]))
                for part, index in ((taken_a, a), (taken_b, b), (made_c, c), (made_d, d)):
                    old = [part[index, rows[v], :] for v in range(BATCH)]
                    for v in range(BATCH):
                        part[index, rows[v], :] = old[v] + rates[v]
                return tuple(heats[v] + heat * rates[v] for v in range(BATCH))

            nothing = tuple(jnp.zeros((8, CZ), jnp.float32) for _ in range(BATCH))
            heats = lax.fori_loop(0, REACTIONS, reaction, nothing, unroll=UNROLL)

            widths = []
            for v in range(BATCH):
                many = counts[rows[v], :]
                live = many > number.astype(jnp.float32)
                width = jnp.where(live, CHEM_STEP / jnp.maximum(many, 1.0), 0.0)
                widths.append(width)
                state[SPECIES, rows[v], :] = state[SPECIES, rows[v], :] + width * heats[v]

            def species(s, carry):
                empty = jnp.zeros((8, CZ), jnp.float32)
                for v in range(BATCH):
                    old = state[s, rows[v], :]
                    lost = widths[v] * (taken_a[s, rows[v], :] + taken_b[s, rows[v], :])
                    gained = widths[v] * (made_c[s, rows[v], :] + made_d[s, rows[v], :])
                    state[s, rows[v], :] = old * ((old + gained) / (old + lost))
                for part in sums:
                    for v in range(BATCH):
                        part[s, rows[v], :] = empty
                return carry

            lax.fori_loop(0, SPECIES, species, 0)
        return carry

    lax.fori_loop(0, SUB, substep, 0)


def second_edge_kernel(
    diffusivity, mechanism, prefactor, activation, heat_release,
    partial, weights, work, xh0, xh1, yh0, yh1, zh0, zh1,
    out, columns, turned, state, counts, sum_a, sum_b, sum_c, sum_d, y_lows, y_highs, sems,
):
    def leaving(group):
        part = pl.ds(group * GROUP, GROUP)
        return pltpu.make_async_copy(state.at[part], out.at[part], sems.at[group])

    columns[...] = jnp.zeros_like(columns)
    columns[0:CX, 0:CY] = work[...]
    turned[...] = columns[...].T
    for x in range(CX):
        counts[x * CY : (x + 1) * CY, :] = jnp.broadcast_to(turned[0:CY, x : x + 1], (CY, CZ))
    turn_halos(zh0, zh1, columns, turned)

    @pl.loop(0, STEPS)
    def _(step):
        block, *halos = group_of((partial, xh0, xh1, yh0, yh1), step)
        (result,) = group_of((state,), step)
        close_group(
            step, block, halos, diffusivity, weights, turned, (y_lows, y_highs), result
        )

    for group in range(3, STEPS):
        leaving(group).start()
    react(
        state, counts, mechanism, prefactor, activation, heat_release,
        (sum_a, sum_b, sum_c, sum_d),
    )
    for group in range(3):
        leaving(group).start()
    for group in range(STEPS):
        leaving(group).wait()


SCALARS = pl.BlockSpec(memory_space=pltpu.SMEM)
WHOLE = pl.BlockSpec(memory_space=pltpu.VMEM)
FAR = pl.BlockSpec(memory_space=pltpu.HBM)
HALO_SHAPES = [
    jax.ShapeDtypeStruct(shape, jnp.float32)
    for shape in (
        (FIELDS, CY, CZ), (FIELDS, CY, CZ), (FIELDS, CX, CZ), (FIELDS, CX, CZ),
        (FIELDS, CZ), (FIELDS, CZ),
    )
]
SQUARE = pltpu.VMEM((ROWS, CZ), jnp.float32)
MIB = 1024 * 1024
FACES_LIMIT = 47 * MIB
INNER_COST = pl.CostEstimate(flops=60_000_000, bytes_accessed=8_000_000, transcendentals=0)


def exchanged_along(k, sends):
    return [swapped(sends[0], AXES[k], 0), swapped(sends[1], AXES[k], 1)]


def exchanged(sends):
    return [half for k in range(3) for half in exchanged_along(k, sends[2 * k : 2 * k + 2])]


def body(
    fields, source, velocity, diffusivity, reacting, counts, mechanism, prefactor, activation,
    heat_release,
):
    fields = fields.reshape(FIELDS, ROWS, CZ)
    source = source.reshape(FIELDS, ROWS, CZ)
    velocity = velocity.reshape(3, ROWS, CZ)
    work = jnp.where(reacting == 1, counts, 0).astype(jnp.float32).reshape(CX, CY)
    all_fields = jax.ShapeDtypeStruct((FIELDS, ROWS, CZ), jnp.float32)
    all_weights = jax.ShapeDtypeStruct((7, ROWS, CZ), jnp.float32)
    y_edges = [pltpu.VMEM((GROUP, CX, CZ), jnp.float32)] * 2

    held, kept, weights, *sends = pl.pallas_call(
        faces_kernel,
        in_specs=[FAR] * 3,
        out_specs=[WHOLE] * 9,
        out_shape=[all_fields, all_fields, all_weights] + HALO_SHAPES,
        scratch_shapes=[
            pltpu.VMEM((3, ROWS, CZ), jnp.float32),
            SQUARE,
            SQUARE,
            pltpu.SemaphoreType.DMA((2 * STEPS + 1,)),
        ],
        compiler_params=pltpu.CompilerParams(vmem_limit_bytes=FACES_LIMIT),
        name="faces",
    )(fields, source, velocity)
    halos = exchanged(sends)
    inner = pl.pallas_call(
        inner_kernel,
        in_specs=[SCALARS] + [WHOLE] * 3,
        out_specs=WHOLE,
        out_shape=all_fields,
        compiler_params=pltpu.CompilerParams(vmem_limit_bytes=12 * MIB),
        cost_estimate=INNER_COST,
        name="inner",
    )
    partial = inner(diffusivity, held, kept, weights)
    moved, *sends = pl.pallas_call(
        first_edge_kernel,
        in_specs=[SCALARS] + [WHOLE] * 8,
        out_specs=[WHOLE] * 7,
        out_shape=[all_fields] + HALO_SHAPES,
        scratch_shapes=[SQUARE] * 4 + y_edges,
        compiler_params=pltpu.CompilerParams(vmem_limit_bytes=12 * MIB),
        name="first_edge",
    )(diffusivity, partial, weights, *halos)
    halos = exchanged(sends)
    partial = inner(diffusivity, moved, kept, weights)
    sums = [pltpu.VMEM((SPECIES, ROWS, CZ), jnp.float32)] * 4
    out = pl.pallas_call(
        second_edge_kernel,
        in_specs=[SCALARS] * 5 + [WHOLE] * 9,
        out_specs=FAR,
        out_shape=all_fields,
        scratch_shapes=[SQUARE, SQUARE, pltpu.VMEM((FIELDS, ROWS, CZ), jnp.float32), SQUARE]
        + sums
        + y_edges
        + [pltpu.SemaphoreType.DMA((STEPS,))],
        compiler_params=pltpu.CompilerParams(vmem_limit_bytes=20 * MIB),
        name="second_edge",
    )(
        diffusivity, mechanism, prefactor, activation, heat_release,
        partial, weights, work, *halos,
    )
    return out.reshape(FIELDS, CX, CY, CZ)


def solution(mesh):
    grid = P(None, "gx", "gy", "gz")
    placed = (
        grid, grid, grid, P(), P("gx", "gy", "gz"), P("gx", "gy", "gz"), P(), P(), P(), P(),
    )
    return jax.shard_map(body, mesh=mesh, in_specs=placed, out_specs=grid, check_vma=False)
```

```python
import jax
import jax.numpy as jnp
from jax import lax
from jax.experimental import pallas as pl
from jax.experimental.pallas import tpu as pltpu
from jax.sharding import PartitionSpec as P

FIELDS = 40
SPECIES = 22
REACTIONS = 100
SUB = 4
FEW = 96
CX = 8
CY = 16
CZ = 128
ROWS = CX * CY
GROUP = 8
STEPS = FIELDS // GROUP
COURANT = 0.15
CHEM_STEP = 0.25
LOG2E = 1.4426950408889634
AXES = ("gx", "gy", "gz")


def place(axis):
    index = lax.axis_index(axis)
    even = lax.rem(index, 2) == 0
    return even, index > 0, index < lax.axis_size(axis) - 1


def swapped(value, axis, start):
    size = lax.axis_size(axis)
    pairs = []
    for low in range(start, size, 2):
        high = (low + 1) % size
        pairs += [(low, high), (high, low)]
    return lax.ppermute(value, axis, pairs)


def x_rows():
    xeven, _, _ = place("gx")
    high = pl.multiple_of(jnp.where(xeven, (CX - 1) * CY, 0), CY)
    low = pl.multiple_of(jnp.where(xeven, 0, (CX - 1) * CY), CY)
    return high, low


def pick_x(block, sends):
    xs0, xs1 = sends
    high, low = x_rows()
    for f in range(GROUP):
        xs0[f] = block[f, pl.ds(high, CY), :]
        xs1[f] = block[f, pl.ds(low, CY), :]


def pick_yz(step, block, sends, columns):
    ys0, ys1 = sends
    yeven, _, _ = place("gy")
    high_y = jnp.where(yeven, CY - 1, 0)
    low_y = jnp.where(yeven, 0, CY - 1)
    for f in range(GROUP):
        ys0[f] = block[f, pl.ds(high_y, CX, stride=CY), :]
        ys1[f] = block[f, pl.ds(low_y, CX, stride=CY), :]
    lane = lax.broadcasted_iota(jnp.int32, (8, CZ), 1)
    first = step * (2 * GROUP)
    for r in range(0, ROWS, 8):
        total = columns[r : r + 8, :]
        for f in range(GROUP):
            moved = pltpu.roll(block[f, r : r + 8, :], first + 2 * f + 1, 1)
            here = lane - first
            total = jnp.where((here >= 2 * f) & (here < 2 * f + 2), moved, total)
        columns[r : r + 8, :] = total


def turn_faces(zs0, zs1, columns, turned):
    zeven, _, _ = place("gz")
    turned[...] = columns[...].T
    highs = turned[pl.ds(0, FIELDS, stride=2), :]
    lows = turned[pl.ds(1, FIELDS, stride=2), :]
    zs0[...] = jnp.where(zeven, highs, lows)
    zs1[...] = jnp.where(zeven, lows, highs)


def group_of(refs, step):
    return [ref.at[pl.ds(step * GROUP, GROUP)] for ref in refs]


def faces_kernel(
    fields, source, held, kept, xs0, xs1, ys0, ys1, zs0, zs1, columns, turned, sems
):
    def arriving(whole, local, step, k):
        part = pl.ds(step * GROUP, GROUP)
        return pltpu.make_async_copy(whole.at[part], local.at[part], sems.at[k + step])

    for step in range(STEPS):
        arriving(fields, held, step, 0).start()
    for step in range(STEPS):
        arriving(source, kept, step, STEPS).start()
    columns[...] = jnp.zeros_like(columns)

    @pl.loop(0, STEPS)
    def _(step):
        arriving(fields, held, step, 0).wait()
        block, *sends = group_of((held, xs0, xs1, ys0, ys1), step)
        pick_x(block, sends[:2])
        pick_yz(step, block, sends[2:], columns)

    turn_faces(zs0, zs1, columns, turned)
    for step in range(STEPS):
        arriving(source, kept, step, STEPS).wait()


def set_up(velocity, weights):
    for r in range(0, ROWS, 8):
        rest = jnp.ones((8, CZ), jnp.float32)
        for a in range(3):
            speed = velocity[a, r : r + 8, :]
            below = COURANT * jnp.maximum(speed, 0.0)
            above = -COURANT * jnp.minimum(speed, 0.0)
            weights[2 * a, r : r + 8, :] = below
            weights[2 * a + 1, r : r + 8, :] = above
            rest = rest - (below + above)
        weights[6, r : r + 8, :] = rest


def move_group(step, block, source, diffusivity, weights, result):
    row = lax.broadcasted_iota(jnp.int32, (CY, CZ), 0)
    lane = lax.broadcasted_iota(jnp.int32, (CY, CZ), 1)
    diffuse = [diffusivity[step * GROUP + f] for f in range(GROUP)]
    for x in range(CX):
        here = slice(x * CY, (x + 1) * CY)
        share = [weights[k, here, :] for k in range(7)]
        for f in range(GROUP):
            cell = block[f, here, :]
            ym = jnp.where(row == 0, 0.0, pltpu.roll(cell, 1, 0))
            yp = jnp.where(row == CY - 1, 0.0, pltpu.roll(cell, CY - 1, 0))
            zm = jnp.where(lane == 0, 0.0, pltpu.roll(cell, 1, 1))
            zp = jnp.where(lane == CZ - 1, 0.0, pltpu.roll(cell, CZ - 1, 1))
            around = (ym + yp) + (zm + zp)
            carried = (share[2] * ym + share[3] * yp) + (share[4] * zm + share[5] * zp)
            if x > 0:
                xm = block[f, (x - 1) * CY : x * CY, :]
                around, carried = around + xm, carried + share[0] * xm
            if x < CX - 1:
                xp = block[f, (x + 1) * CY : (x + 2) * CY, :]
                around, carried = around + xp, carried + share[1] * xp
            kept = cell * (share[6] - 6.0 * diffuse[f])
            result[f, here, :] = (kept + source[f, here, :]) + (carried + diffuse[f] * around)


def turn_halos(zh0, zh1, columns, turned):
    zeven, has_low, has_high = place("gz")
    columns[...] = jnp.zeros_like(columns)
    first, second = zh0[...], zh1[...]
    high = jnp.where(has_high, jnp.where(zeven, first, second), 0.0)
    low = jnp.where(has_low, jnp.where(zeven, second, first), 0.0)
    columns[pl.ds(0, FIELDS, stride=2), :] = high
    columns[pl.ds(1, FIELDS, stride=2), :] = low
    turned[...] = columns[...].T


def close_group(step, partial, halos, diffusivity, weights, turned, y_edges, result):
    xh0, xh1, yh0, yh1 = halos
    y_lows, y_highs = y_edges
    xeven, x_low, x_high = place("gx")
    yeven, y_low, y_high = place("gy")
    row = lax.broadcasted_iota(jnp.int32, (8, CZ), 0)
    lane = lax.broadcasted_iota(jnp.int32, (8, CZ), 1)
    one_low = jnp.where(row == 0, 1.0, 0.0)
    one_high = jnp.where(row == 7, 1.0, 0.0)
    one_z = jnp.where((lane == 0) | (lane == CZ - 1), 1.0, 0.0)
    diffuse = [diffusivity[step * GROUP + f] for f in range(GROUP)]
    for f in range(GROUP):
        first, second = yh0[f], yh1[f]
        y_lows[f] = jnp.where(y_low, jnp.where(yeven, second, first), 0.0)
        y_highs[f] = jnp.where(y_high, jnp.where(yeven, first, second), 0.0)
    for x in range(CX):
        for half in range(2):
            here = slice(x * CY + 8 * half, x * CY + 8 * half + 8)
            part = slice(8 * half, 8 * half + 8)
            edge = turned[here, :]
            share_y = weights[2 + half, here, :] * (one_high if half else one_low)
            share_z = jnp.where(
                lane == 0,
                weights[4, here, :],
                jnp.where(lane == CZ - 1, weights[5, here, :], 0.0),
            )
            for f in range(GROUP):
                y_near = (y_highs if half else y_lows)[f, x : x + 1, :]
                z_near = pltpu.roll(edge, CZ - 1 - 2 * f - step * (2 * GROUP), 1)
                one_y = one_high if half else one_low
                more = (share_y + diffuse[f] * one_y) * y_near
                more = more + (share_z + diffuse[f] * one_z) * z_near
                if x == 0:
                    near = jnp.where(xeven, xh1[f, part, :], xh0[f, part, :])
                    near = jnp.where(x_low, near, 0.0)
                    more = more + (weights[0, here, :] + diffuse[f]) * near
                if x == CX - 1:
                    near = jnp.where(xeven, xh0[f, part, :], xh1[f, part, :])
                    near = jnp.where(x_high, near, 0.0)
                    more = more + (weights[1, here, :] + diffuse[f]) * near
                result[f, here, :] = partial[f, here, :] + more


def first_edge_kernel(
    diffusivity, partial, weights, xh0, xh1, yh0, yh1, zh0, zh1,
    moved, xs0, xs1, ys0, ys1, zs0, zs1, columns, turned, faces, across, y_lows, y_highs,
):
    turn_halos(zh0, zh1, columns, turned)
    faces[...] = jnp.zeros_like(faces)

    @pl.loop(0, STEPS)
    def _(step):
        block, *halos = group_of((partial, xh0, xh1, yh0, yh1), step)
        (result,) = group_of((moved,), step)
        close_group(
            step, block, halos, diffusivity, weights, turned, (y_lows, y_highs), result
        )

    @pl.loop(0, STEPS)
    def _(step):
        result, *sends = group_of((moved, xs0, xs1, ys0, ys1), step)
        pick_x(result, sends[:2])
        pick_yz(step, result, sends[2:], faces)

    turn_faces(zs0, zs1, faces, across)


def first_inner_kernel(diffusivity, fields, source, velocity, partial, weights):
    set_up(velocity, weights)
    inner_kernel(diffusivity, fields, source, weights, partial)


def inner_kernel(diffusivity, fields, source, weights, partial):
    @pl.loop(0, STEPS)
    def _(step):
        block, more, result = group_of((fields, source, partial), step)
        move_group(step, block, more, diffusivity, weights, result)


def rank_blocks(counts, table):
    row = lax.broadcasted_iota(jnp.int32, (ROWS, CZ), 0)
    lane = lax.broadcasted_iota(jnp.int32, (ROWS, CZ), 1)
    mine = counts[...]
    other = mine.T
    ahead = (mine > other) | ((mine == other) & (row < lane))
    ranks = jnp.sum(jnp.where(ahead, 1.0, 0.0), axis=0, keepdims=True)
    down = jnp.broadcast_to(ranks, (ROWS, CZ)).T
    chosen = down == lane.astype(jnp.float32)
    order = jnp.sum(jnp.where(chosen, row.astype(jnp.float32), 0.0), axis=0, keepdims=True)
    longer = jnp.where(mine > lane.astype(jnp.float32), 1.0, 0.0)
    longer = jnp.sum(longer, axis=0, keepdims=True)
    table[0:1, :] = ranks.astype(jnp.int32)
    table[1:2, :] = order.astype(jnp.int32)
    table[2:3, :] = longer.astype(jnp.int32)


def gather_rows(source, target, group, index):
    row = lax.broadcasted_iota(jnp.int32, (8, CZ), 0)
    here = pl.ds(pl.multiple_of(8 * group, 8), 8)
    picks = [index(8 * group + r) for r in range(8)]
    for s in range(SPECIES + 1):
        total = jnp.broadcast_to(source[s, pl.ds(picks[0], 1), :], (8, CZ))
        for r in range(1, 8):
            total = jnp.where(row == r, source[s, pl.ds(picks[r], 1), :], total)
        target[s, here, :] = total


def react_rows(base, size, unroll, width_of, state, reactions, sums, finish=None):
    mechanism, prefactor, activation, heat_release = reactions
    taken_a, taken_b, made_c, made_d = sums
    rows = [pl.ds(base + 8 * v, 8) for v in range(size)]
    cold = [1.0 / state[SPECIES, r, :] for r in rows]

    def reaction(j, heats):
        a, b = mechanism[0, j], mechanism[1, j]
        c, d = mechanism[2, j], mechanism[3, j]
        strength, heat = prefactor[j], heat_release[j]
        barrier = -LOG2E * activation[j]
        rates = []
        for v in range(size):
            rate = strength * jnp.exp2(barrier * cold[v])
            rates.append(rate * (state[a, rows[v], :] * state[b, rows[v], :]))
        for part, index in ((taken_a, a), (taken_b, b), (made_c, c), (made_d, d)):
            old = [part[index, rows[v], :] for v in range(size)]
            for v in range(size):
                part[index, rows[v], :] = old[v] + rates[v]
        return tuple(heats[v] + heat * rates[v] for v in range(size))

    nothing = tuple(jnp.zeros((8, CZ), jnp.float32) for _ in range(size))
    heats = lax.fori_loop(0, REACTIONS, reaction, nothing, unroll=unroll)

    widths = []
    for v in range(size):
        width = width_of(rows[v], base + 8 * v)
        widths.append(width)
        state[SPECIES, rows[v], :] = state[SPECIES, rows[v], :] + width * heats[v]
    if finish is not None:
        finish(SPECIES)

    def species(s, carry):
        empty = jnp.zeros((8, CZ), jnp.float32)
        for v in range(size):
            old = state[s, rows[v], :]
            lost = widths[v] * (taken_a[s, rows[v], :] + taken_b[s, rows[v], :])
            gained = widths[v] * (made_c[s, rows[v], :] + made_d[s, rows[v], :])
            state[s, rows[v], :] = old * ((old + gained) / (old + lost))
        for part in sums:
            for v in range(size):
                part[s, rows[v], :] = empty
        if finish is not None:
            finish(s)
        return carry

    lax.fori_loop(0, SPECIES, species, 0)

def react_sorted(state, order, reactions, sums):
    @pl.loop(0, SUB)
    def _(number):
        def width_of(rows, low):
            place = lax.broadcasted_iota(jnp.int32, (8, CZ), 0) + low
            many = jnp.ones((8, CZ), jnp.float32)
            for k in range(1, SUB):
                many = many + jnp.where(place < order[2, k], 1.0, 0.0)
            return jnp.where(place < order[2, number], CHEM_STEP / many, 0.0)

        active = order[2, number]
        large = lax.shift_right_logical(active + 31, 6)

        @pl.loop(0, large)
        def _(k):
            base = pl.multiple_of(k * 64, 64)
            react_rows(base, 8, 4, width_of, state, reactions, sums)

        @pl.when(active > large * 64)
        def _():
            base = pl.multiple_of(large * 64, 64)
            react_rows(base, 4, 5, width_of, state, reactions, sums)


def react_all(state, counts, reactions, sums, leave):
    @pl.loop(0, SUB)
    def _(number):
        def width_of(rows, low):
            many = counts[rows, :]
            live = many > number.astype(jnp.float32)
            return jnp.where(live, CHEM_STEP / jnp.maximum(many, 1.0), 0.0)

        def finish(s):
            @pl.when(number == SUB - 1)
            def _():
                leave(s).start()

        react_rows(0, ROWS // 8, 2, width_of, state, reactions, sums, finish)


def second_edge_kernel(
    diffusivity, mechanism, prefactor, activation, heat_release,
    partial, weights, work, xh0, xh1, yh0, yh1, zh0, zh1,
    out, columns, turned, state, counts, ordered, sum_a, sum_b, sum_c, sum_d, y_lows, y_highs,
    table, order, sems,
):
    def leaving(low, many, k):
        part = pl.ds(low, many)
        return pltpu.make_async_copy(state.at[part], out.at[part], sems.at[k])

    columns[...] = jnp.zeros_like(columns)
    columns[0:CX, 0:CY] = work[...]
    turned[...] = columns[...].T
    for x in range(CX):
        counts[x * CY : (x + 1) * CY, :] = jnp.broadcast_to(turned[0:CY, x : x + 1], (CY, CZ))
    rank_blocks(counts, table)
    listing = pltpu.make_async_copy(table, order, sems.at[0])
    listing.start()
    turn_halos(zh0, zh1, columns, turned)

    @pl.loop(0, STEPS)
    def _(step):
        block, *halos = group_of((partial, xh0, xh1, yh0, yh1), step)
        (result,) = group_of((state,), step)
        for part in (sum_a, sum_b, sum_c, sum_d):
            for k in range(5):
                s = jnp.minimum(5 * step + k, SPECIES - 1)
                part[s] = jnp.zeros((ROWS, CZ), jnp.float32)
        close_group(
            step, block, halos, diffusivity, weights, turned, (y_lows, y_highs), result
        )

    listing.wait()
    rest = leaving(SPECIES + 1, FIELDS - SPECIES - 1, 1)
    rest.start()

    reactions = (mechanism, prefactor, activation, heat_release)
    sums = (sum_a, sum_b, sum_c, sum_d)
    few = order[2, 0] <= FEW

    @pl.when(few)
    def _():
        @pl.loop(0, ROWS // 8)
        def _(group):
            gather_rows(state, ordered, group, lambda p: order[1, p])

        react_sorted(ordered, order, reactions, sums)

        @pl.loop(0, ROWS // 8)
        def _(group):
            gather_rows(ordered, state, group, lambda p: order[0, p])

        @pl.loop(0, SPECIES + 1)
        def _(s):
            leaving(s, 1, 2).start()

    @pl.when(jnp.logical_not(few))
    def _():
        react_all(state, counts, reactions, sums, lambda s: leaving(s, 1, 2))

    rest.wait()
    leaving(0, SPECIES + 1, 2).wait()


SCALARS = pl.BlockSpec(memory_space=pltpu.SMEM)
WHOLE = pl.BlockSpec(memory_space=pltpu.VMEM)
FAR = pl.BlockSpec(memory_space=pltpu.HBM)
HALO_SHAPES = [
    jax.ShapeDtypeStruct(shape, jnp.float32)
    for shape in (
        (FIELDS, CY, CZ), (FIELDS, CY, CZ), (FIELDS, CX, CZ), (FIELDS, CX, CZ),
        (FIELDS, CZ), (FIELDS, CZ),
    )
]
SQUARE = pltpu.VMEM((ROWS, CZ), jnp.float32)
MIB = 1024 * 1024
FACES_LIMIT = 47 * MIB
INNER_COST = pl.CostEstimate(flops=60_000_000, bytes_accessed=8_000_000, transcendentals=0)


def exchanged_along(k, sends):
    return [swapped(sends[0], AXES[k], 0), swapped(sends[1], AXES[k], 1)]


def exchanged(sends):
    return [half for k in range(3) for half in exchanged_along(k, sends[2 * k : 2 * k + 2])]


def body(
    fields, source, velocity, diffusivity, reacting, counts, mechanism, prefactor, activation,
    heat_release,
):
    fields = fields.reshape(FIELDS, ROWS, CZ)
    source = source.reshape(FIELDS, ROWS, CZ)
    velocity = velocity.reshape(3, ROWS, CZ)
    work = jnp.where(reacting == 1, counts, 0).astype(jnp.float32).reshape(CX, CY)
    all_fields = jax.ShapeDtypeStruct((FIELDS, ROWS, CZ), jnp.float32)
    all_weights = jax.ShapeDtypeStruct((7, ROWS, CZ), jnp.float32)
    y_edges = [pltpu.VMEM((GROUP, CX, CZ), jnp.float32)] * 2

    held, kept, *sends = pl.pallas_call(
        faces_kernel,
        in_specs=[FAR] * 2,
        out_specs=[WHOLE] * 8,
        out_shape=[all_fields, all_fields] + HALO_SHAPES,
        scratch_shapes=[SQUARE, SQUARE, pltpu.SemaphoreType.DMA((2 * STEPS,))],
        compiler_params=pltpu.CompilerParams(vmem_limit_bytes=FACES_LIMIT),
        name="faces",
    )(fields, source)
    halos = exchanged(sends)
    partial, weights = pl.pallas_call(
        first_inner_kernel,
        in_specs=[SCALARS] + [WHOLE] * 3,
        out_specs=[WHOLE] * 2,
        out_shape=[all_fields, all_weights],
        compiler_params=pltpu.CompilerParams(vmem_limit_bytes=12 * MIB),
        cost_estimate=INNER_COST,
        name="first_inner",
    )(diffusivity, held, kept, velocity)
    moved, *sends = pl.pallas_call(
        first_edge_kernel,
        in_specs=[SCALARS] + [WHOLE] * 8,
        out_specs=[WHOLE] * 7,
        out_shape=[all_fields] + HALO_SHAPES,
        scratch_shapes=[SQUARE] * 4 + y_edges,
        compiler_params=pltpu.CompilerParams(vmem_limit_bytes=12 * MIB),
        name="first_edge",
    )(diffusivity, partial, weights, *halos)
    halos = exchanged(sends)
    partial = pl.pallas_call(
        inner_kernel,
        in_specs=[SCALARS] + [WHOLE] * 3,
        out_specs=WHOLE,
        out_shape=all_fields,
        compiler_params=pltpu.CompilerParams(vmem_limit_bytes=12 * MIB),
        cost_estimate=INNER_COST,
        name="second_inner",
    )(diffusivity, moved, kept, weights)
    sums = [pltpu.VMEM((SPECIES, ROWS, CZ), jnp.float32)] * 4
    out = pl.pallas_call(
        second_edge_kernel,
        in_specs=[SCALARS] * 5 + [WHOLE] * 9,
        out_specs=FAR,
        out_shape=all_fields,
        scratch_shapes=[SQUARE, SQUARE, pltpu.VMEM((FIELDS, ROWS, CZ), jnp.float32), SQUARE]
        + [pltpu.VMEM((SPECIES + 1, ROWS, CZ), jnp.float32)]
        + sums
        + y_edges
        + [
            pltpu.VMEM((8, CZ), jnp.int32),
            pltpu.SMEM((8, CZ), jnp.int32),
            pltpu.SemaphoreType.DMA((3,)),
        ],
        compiler_params=pltpu.CompilerParams(vmem_limit_bytes=20 * MIB),
        name="second_edge",
    )(
        diffusivity, mechanism, prefactor, activation, heat_release,
        partial, weights, work, *halos,
    )
    return out.reshape(FIELDS, CX, CY, CZ)


def solution(mesh):
    grid = P(None, "gx", "gy", "gz")
    placed = (
        grid, grid, grid, P(), P("gx", "gy", "gz"), P("gx", "gy", "gz"), P(), P(), P(), P(),
    )
    return jax.shard_map(body, mesh=mesh, in_specs=placed, out_specs=grid, check_vma=False)
```

```python
import jax
import jax.numpy as jnp
from jax import lax
from jax.experimental import pallas as pl
from jax.experimental.pallas import tpu as pltpu
from jax.sharding import PartitionSpec as P

FIELDS = 40
SPECIES = 22
REACTIONS = 100
SUB = 4
FEW = 96
CX = 8
CY = 16
CZ = 128
ROWS = CX * CY
GROUP = 8
STEPS = FIELDS // GROUP
COURANT = 0.15
CHEM_STEP = 0.25
LOG2E = 1.4426950408889634
AXES = ("gx", "gy", "gz")


def place(axis):
    index = lax.axis_index(axis)
    even = lax.rem(index, 2) == 0
    return even, index > 0, index < lax.axis_size(axis) - 1


def swapped(value, axis, start):
    size = lax.axis_size(axis)
    pairs = []
    for low in range(start, size, 2):
        high = (low + 1) % size
        pairs += [(low, high), (high, low)]
    return lax.ppermute(value, axis, pairs)


def x_rows():
    xeven, _, _ = place("gx")
    high = pl.multiple_of(jnp.where(xeven, (CX - 1) * CY, 0), CY)
    low = pl.multiple_of(jnp.where(xeven, 0, (CX - 1) * CY), CY)
    return high, low


def pick_x(block, sends):
    xs0, xs1 = sends
    high, low = x_rows()
    for f in range(GROUP):
        xs0[f] = block[f, pl.ds(high, CY), :]
        xs1[f] = block[f, pl.ds(low, CY), :]


def pick_yz(step, block, sends, columns):
    ys0, ys1 = sends
    yeven, _, _ = place("gy")
    high_y = jnp.where(yeven, CY - 1, 0)
    low_y = jnp.where(yeven, 0, CY - 1)
    for f in range(GROUP):
        ys0[f] = block[f, pl.ds(high_y, CX, stride=CY), :]
        ys1[f] = block[f, pl.ds(low_y, CX, stride=CY), :]
    lane = lax.broadcasted_iota(jnp.int32, (8, CZ), 1)
    first = step * (2 * GROUP)
    for r in range(0, ROWS, 8):
        total = columns[r : r + 8, :]
        for f in range(GROUP):
            moved = pltpu.roll(block[f, r : r + 8, :], first + 2 * f + 1, 1)
            here = lane - first
            total = jnp.where((here >= 2 * f) & (here < 2 * f + 2), moved, total)
        columns[r : r + 8, :] = total


def turn_faces(zs0, zs1, columns, turned):
    zeven, _, _ = place("gz")
    turned[...] = columns[...].T
    highs = turned[pl.ds(0, FIELDS, stride=2), :]
    lows = turned[pl.ds(1, FIELDS, stride=2), :]
    zs0[...] = jnp.where(zeven, highs, lows)
    zs1[...] = jnp.where(zeven, lows, highs)


def group_of(refs, step):
    return [ref.at[pl.ds(step * GROUP, GROUP)] for ref in refs]


def faces_kernel(
    fields, source, held, kept, xs0, xs1, ys0, ys1, zs0, zs1, columns, turned, sems
):
    def arriving(whole, local, step, k):
        part = pl.ds(step * GROUP, GROUP)
        return pltpu.make_async_copy(whole.at[part], local.at[part], sems.at[k + step])

    for step in range(STEPS):
        arriving(fields, held, step, 0).start()
    for step in range(STEPS):
        arriving(source, kept, step, STEPS).start()
    columns[...] = jnp.zeros_like(columns)

    @pl.loop(0, STEPS)
    def _(step):
        arriving(fields, held, step, 0).wait()
        block, *sends = group_of((held, xs0, xs1, ys0, ys1), step)
        pick_x(block, sends[:2])
        pick_yz(step, block, sends[2:], columns)

    turn_faces(zs0, zs1, columns, turned)
    for step in range(STEPS):
        arriving(source, kept, step, STEPS).wait()


def set_up(velocity, weights):
    for r in range(0, ROWS, 8):
        rest = jnp.ones((8, CZ), jnp.float32)
        for a in range(3):
            speed = velocity[a, r : r + 8, :]
            below = COURANT * jnp.maximum(speed, 0.0)
            above = -COURANT * jnp.minimum(speed, 0.0)
            weights[2 * a, r : r + 8, :] = below
            weights[2 * a + 1, r : r + 8, :] = above
            rest = rest - (below + above)
        weights[6, r : r + 8, :] = rest


def move_group(step, block, source, diffusivity, weights, result):
    row = lax.broadcasted_iota(jnp.int32, (8, CZ), 0)
    lane = lax.broadcasted_iota(jnp.int32, (8, CZ), 1)
    diffuse = [diffusivity[step * GROUP + f] for f in range(GROUP)]
    for low in range(0, ROWS, 8):
        here = slice(low, low + 8)
        before, after = slice(low - 1, low + 7), slice(low + 1, low + 9)
        share = [weights[k, here, :] for k in range(7)]
        size = [share[2 * a] + share[2 * a + 1] for a in range(3)]
        rising = [share[2 * a] > 0.0 for a in range(3)]
        for f in range(GROUP):
            cell = block[f, here, :]
            ym = block[f, before, :] if low > 0 else pltpu.roll(cell, 1, 0)
            yp = block[f, after, :] if low < ROWS - 8 else pltpu.roll(cell, 7, 0)
            if low % CY == 0:
                ym = jnp.where(row == 0, 0.0, ym)
            else:
                yp = jnp.where(row == 7, 0.0, yp)
            zm = jnp.where(lane == 0, 0.0, pltpu.roll(cell, 1, 1))
            zp = jnp.where(lane == CZ - 1, 0.0, pltpu.roll(cell, CZ - 1, 1))
            around = (ym + yp) + (zm + zp)
            carried = size[1] * jnp.where(rising[1], ym, yp)
            carried = carried + size[2] * jnp.where(rising[2], zm, zp)
            if low < CY:
                xp = block[f, low + CY : low + CY + 8, :]
                around, carried = around + xp, carried + share[1] * xp
            elif low >= ROWS - CY:
                xm = block[f, low - CY : low - CY + 8, :]
                around, carried = around + xm, carried + share[0] * xm
            else:
                xm = block[f, low - CY : low - CY + 8, :]
                xp = block[f, low + CY : low + CY + 8, :]
                around = around + (xm + xp)
                carried = carried + size[0] * jnp.where(rising[0], xm, xp)
            kept = cell * (share[6] - 6.0 * diffuse[f])
            result[f, here, :] = (kept + source[f, here, :]) + (carried + diffuse[f] * around)


def turn_halos(zh0, zh1, columns, turned):
    zeven, has_low, has_high = place("gz")
    columns[...] = jnp.zeros_like(columns)
    first, second = zh0[...], zh1[...]
    high = jnp.where(has_high, jnp.where(zeven, first, second), 0.0)
    low = jnp.where(has_low, jnp.where(zeven, second, first), 0.0)
    columns[pl.ds(0, FIELDS, stride=2), :] = high
    columns[pl.ds(1, FIELDS, stride=2), :] = low
    turned[...] = columns[...].T


def close_group(step, partial, halos, diffusivity, weights, turned, y_edges, result):
    xh0, xh1, yh0, yh1 = halos
    y_lows, y_highs = y_edges
    xeven, x_low, x_high = place("gx")
    yeven, y_low, y_high = place("gy")
    row = lax.broadcasted_iota(jnp.int32, (8, CZ), 0)
    lane = lax.broadcasted_iota(jnp.int32, (8, CZ), 1)
    one_low = jnp.where(row == 0, 1.0, 0.0)
    one_high = jnp.where(row == 7, 1.0, 0.0)
    one_z = jnp.where((lane == 0) | (lane == CZ - 1), 1.0, 0.0)
    diffuse = [diffusivity[step * GROUP + f] for f in range(GROUP)]
    for f in range(GROUP):
        first, second = yh0[f], yh1[f]
        y_lows[f] = jnp.where(y_low, jnp.where(yeven, second, first), 0.0)
        y_highs[f] = jnp.where(y_high, jnp.where(yeven, first, second), 0.0)
    for x in range(CX):
        for half in range(2):
            here = slice(x * CY + 8 * half, x * CY + 8 * half + 8)
            part = slice(8 * half, 8 * half + 8)
            edge = turned[here, :]
            share_y = weights[2 + half, here, :] * (one_high if half else one_low)
            share_z = jnp.where(
                lane == 0,
                weights[4, here, :],
                jnp.where(lane == CZ - 1, weights[5, here, :], 0.0),
            )
            for f in range(GROUP):
                y_near = (y_highs if half else y_lows)[f, x : x + 1, :]
                z_near = pltpu.roll(edge, CZ - 1 - 2 * f - step * (2 * GROUP), 1)
                one_y = one_high if half else one_low
                more = (share_y + diffuse[f] * one_y) * y_near
                more = more + (share_z + diffuse[f] * one_z) * z_near
                if x == 0:
                    near = jnp.where(xeven, xh1[f, part, :], xh0[f, part, :])
                    near = jnp.where(x_low, near, 0.0)
                    more = more + (weights[0, here, :] + diffuse[f]) * near
                if x == CX - 1:
                    near = jnp.where(xeven, xh0[f, part, :], xh1[f, part, :])
                    near = jnp.where(x_high, near, 0.0)
                    more = more + (weights[1, here, :] + diffuse[f]) * near
                result[f, here, :] = partial[f, here, :] + more


def first_edge_kernel(
    diffusivity, partial, weights, xh0, xh1, yh0, yh1, zh0, zh1,
    moved, xs0, xs1, ys0, ys1, zs0, zs1, columns, turned, faces, across, y_lows, y_highs,
):
    turn_halos(zh0, zh1, columns, turned)
    faces[...] = jnp.zeros_like(faces)

    @pl.loop(0, STEPS)
    def _(step):
        block, *halos = group_of((partial, xh0, xh1, yh0, yh1), step)
        (result,) = group_of((moved,), step)
        close_group(
            step, block, halos, diffusivity, weights, turned, (y_lows, y_highs), result
        )

    @pl.loop(0, STEPS)
    def _(step):
        result, *sends = group_of((moved, xs0, xs1, ys0, ys1), step)
        pick_x(result, sends[:2])
        pick_yz(step, result, sends[2:], faces)

    turn_faces(zs0, zs1, faces, across)


def first_inner_kernel(diffusivity, fields, source, velocity, partial, weights):
    set_up(velocity, weights)
    inner_kernel(diffusivity, fields, source, weights, partial)


def inner_kernel(diffusivity, fields, source, weights, partial):
    @pl.loop(0, STEPS)
    def _(step):
        block, more, result = group_of((fields, source, partial), step)
        move_group(step, block, more, diffusivity, weights, result)


def rank_blocks(counts, table):
    row = lax.broadcasted_iota(jnp.int32, (ROWS, CZ), 0)
    lane = lax.broadcasted_iota(jnp.int32, (ROWS, CZ), 1)
    mine = counts[...]
    other = mine.T
    ahead = (mine > other) | ((mine == other) & (row < lane))
    ranks = jnp.sum(jnp.where(ahead, 1.0, 0.0), axis=0, keepdims=True)
    down = jnp.broadcast_to(ranks, (ROWS, CZ)).T
    chosen = down == lane.astype(jnp.float32)
    order = jnp.sum(jnp.where(chosen, row.astype(jnp.float32), 0.0), axis=0, keepdims=True)
    longer = jnp.where(mine > lane.astype(jnp.float32), 1.0, 0.0)
    longer = jnp.sum(longer, axis=0, keepdims=True)
    table[0:1, :] = ranks.astype(jnp.int32)
    table[1:2, :] = order.astype(jnp.int32)
    table[2:3, :] = longer.astype(jnp.int32)


def gather_rows(source, target, group, index):
    row = lax.broadcasted_iota(jnp.int32, (8, CZ), 0)
    here = pl.ds(pl.multiple_of(8 * group, 8), 8)
    picks = [index(8 * group + r) for r in range(8)]
    for s in range(SPECIES + 1):
        total = jnp.broadcast_to(source[s, pl.ds(picks[0], 1), :], (8, CZ))
        for r in range(1, 8):
            total = jnp.where(row == r, source[s, pl.ds(picks[r], 1), :], total)
        target[s, here, :] = total


def react_rows(base, size, unroll, width_of, state, reactions, sums, finish=None):
    mechanism, prefactor, activation, heat_release = reactions
    taken_a, taken_b, made_c, made_d = sums
    rows = [pl.ds(base + 8 * v, 8) for v in range(size)]
    cold = [1.0 / state[SPECIES, r, :] for r in rows]

    def reaction(j, heats):
        a, b = mechanism[0, j], mechanism[1, j]
        c, d = mechanism[2, j], mechanism[3, j]
        strength, heat = prefactor[j], heat_release[j]
        barrier = -LOG2E * activation[j]
        rates = []
        for v in range(size):
            rate = strength * jnp.exp2(barrier * cold[v])
            rates.append(rate * (state[a, rows[v], :] * state[b, rows[v], :]))
        for part, index in ((taken_a, a), (taken_b, b), (made_c, c), (made_d, d)):
            old = [part[index, rows[v], :] for v in range(size)]
            for v in range(size):
                part[index, rows[v], :] = old[v] + rates[v]
        return tuple(heats[v] + heat * rates[v] for v in range(size))

    nothing = tuple(jnp.zeros((8, CZ), jnp.float32) for _ in range(size))
    heats = lax.fori_loop(0, REACTIONS, reaction, nothing, unroll=unroll)

    widths = []
    for v in range(size):
        width = width_of(rows[v], base + 8 * v)
        widths.append(width)
        state[SPECIES, rows[v], :] = state[SPECIES, rows[v], :] + width * heats[v]
    if finish is not None:
        finish(SPECIES)

    def species(s, carry):
        empty = jnp.zeros((8, CZ), jnp.float32)
        for v in range(size):
            old = state[s, rows[v], :]
            lost = widths[v] * (taken_a[s, rows[v], :] + taken_b[s, rows[v], :])
            gained = widths[v] * (made_c[s, rows[v], :] + made_d[s, rows[v], :])
            state[s, rows[v], :] = old * ((old + gained) / (old + lost))
        for part in sums:
            for v in range(size):
                part[s, rows[v], :] = empty
        if finish is not None:
            finish(s)
        return carry

    lax.fori_loop(0, SPECIES, species, 0)

def react_sorted(state, order, reactions, sums):
    @pl.loop(0, SUB)
    def _(number):
        def width_of(rows, low):
            place = lax.broadcasted_iota(jnp.int32, (8, CZ), 0) + low
            many = jnp.ones((8, CZ), jnp.float32)
            for k in range(1, SUB):
                many = many + jnp.where(place < order[2, k], 1.0, 0.0)
            return jnp.where(place < order[2, number], CHEM_STEP / many, 0.0)

        active = order[2, number]
        large = lax.shift_right_logical(active + 31, 6)

        @pl.loop(0, large)
        def _(k):
            base = pl.multiple_of(k * 64, 64)
            react_rows(base, 8, 4, width_of, state, reactions, sums)

        @pl.when(active > large * 64)
        def _():
            base = pl.multiple_of(large * 64, 64)
            react_rows(base, 4, 5, width_of, state, reactions, sums)


def react_all(state, counts, reactions, sums, leave):
    @pl.loop(0, SUB)
    def _(number):
        def width_of(rows, low):
            many = counts[rows, :]
            live = many > number.astype(jnp.float32)
            return jnp.where(live, CHEM_STEP / jnp.maximum(many, 1.0), 0.0)

        def finish(s):
            @pl.when(number == SUB - 1)
            def _():
                leave(s).start()

        react_rows(0, ROWS // 8, 4, width_of, state, reactions, sums, finish)


def second_edge_kernel(
    diffusivity, mechanism, prefactor, activation, heat_release,
    partial, weights, work, xh0, xh1, yh0, yh1, zh0, zh1,
    out, columns, turned, state, counts, ordered, sum_a, sum_b, sum_c, sum_d, y_lows, y_highs,
    table, order, sems,
):
    def leaving(low, many, k):
        part = pl.ds(low, many)
        return pltpu.make_async_copy(state.at[part], out.at[part], sems.at[k])

    columns[...] = jnp.zeros_like(columns)
    columns[0:CX, 0:CY] = work[...]
    turned[...] = columns[...].T
    for x in range(CX):
        counts[x * CY : (x + 1) * CY, :] = jnp.broadcast_to(turned[0:CY, x : x + 1], (CY, CZ))
    rank_blocks(counts, table)
    listing = pltpu.make_async_copy(table, order, sems.at[0])
    listing.start()
    turn_halos(zh0, zh1, columns, turned)

    @pl.loop(0, STEPS)
    def _(step):
        block, *halos = group_of((partial, xh0, xh1, yh0, yh1), step)
        (result,) = group_of((state,), step)
        for part in (sum_a, sum_b, sum_c, sum_d):
            for k in range(5):
                s = jnp.minimum(5 * step + k, SPECIES - 1)
                part[s] = jnp.zeros((ROWS, CZ), jnp.float32)
        close_group(
            step, block, halos, diffusivity, weights, turned, (y_lows, y_highs), result
        )

    listing.wait()
    rest = leaving(SPECIES + 1, FIELDS - SPECIES - 1, 1)
    rest.start()

    reactions = (mechanism, prefactor, activation, heat_release)
    sums = (sum_a, sum_b, sum_c, sum_d)
    few = order[2, 0] <= FEW

    @pl.when(few)
    def _():
        @pl.loop(0, ROWS // 8)
        def _(group):
            gather_rows(state, ordered, group, lambda p: order[1, p])

        react_sorted(ordered, order, reactions, sums)

        @pl.loop(0, ROWS // 8)
        def _(group):
            gather_rows(ordered, state, group, lambda p: order[0, p])

        @pl.loop(0, SPECIES + 1)
        def _(s):
            leaving(s, 1, 2).start()

    @pl.when(jnp.logical_not(few))
    def _():
        react_all(state, counts, reactions, sums, lambda s: leaving(s, 1, 2))

    rest.wait()
    leaving(0, SPECIES + 1, 2).wait()


SCALARS = pl.BlockSpec(memory_space=pltpu.SMEM)
WHOLE = pl.BlockSpec(memory_space=pltpu.VMEM)
FAR = pl.BlockSpec(memory_space=pltpu.HBM)
HALO_SHAPES = [
    jax.ShapeDtypeStruct(shape, jnp.float32)
    for shape in (
        (FIELDS, CY, CZ), (FIELDS, CY, CZ), (FIELDS, CX, CZ), (FIELDS, CX, CZ),
        (FIELDS, CZ), (FIELDS, CZ),
    )
]
SQUARE = pltpu.VMEM((ROWS, CZ), jnp.float32)
MIB = 1024 * 1024
FACES_LIMIT = 47 * MIB
INNER_COST = pl.CostEstimate(flops=60_000_000, bytes_accessed=8_000_000, transcendentals=0)


def exchanged_along(k, sends):
    return [swapped(sends[0], AXES[k], 0), swapped(sends[1], AXES[k], 1)]


def exchanged(sends):
    return [half for k in range(3) for half in exchanged_along(k, sends[2 * k : 2 * k + 2])]


def body(
    fields, source, velocity, diffusivity, reacting, counts, mechanism, prefactor, activation,
    heat_release,
):
    fields = fields.reshape(FIELDS, ROWS, CZ)
    source = source.reshape(FIELDS, ROWS, CZ)
    velocity = velocity.reshape(3, ROWS, CZ)
    work = jnp.where(reacting == 1, counts, 0).astype(jnp.float32).reshape(CX, CY)
    all_fields = jax.ShapeDtypeStruct((FIELDS, ROWS, CZ), jnp.float32)
    all_weights = jax.ShapeDtypeStruct((7, ROWS, CZ), jnp.float32)
    y_edges = [pltpu.VMEM((GROUP, CX, CZ), jnp.float32)] * 2

    held, kept, *sends = pl.pallas_call(
        faces_kernel,
        in_specs=[FAR] * 2,
        out_specs=[WHOLE] * 8,
        out_shape=[all_fields, all_fields] + HALO_SHAPES,
        scratch_shapes=[SQUARE, SQUARE, pltpu.SemaphoreType.DMA((2 * STEPS,))],
        compiler_params=pltpu.CompilerParams(vmem_limit_bytes=FACES_LIMIT),
        name="faces",
    )(fields, source)
    halos = exchanged(sends)
    partial, weights = pl.pallas_call(
        first_inner_kernel,
        in_specs=[SCALARS] + [WHOLE] * 3,
        out_specs=[WHOLE] * 2,
        out_shape=[all_fields, all_weights],
        compiler_params=pltpu.CompilerParams(vmem_limit_bytes=12 * MIB),
        cost_estimate=INNER_COST,
        name="first_inner",
    )(diffusivity, held, kept, velocity)
    moved, *sends = pl.pallas_call(
        first_edge_kernel,
        in_specs=[SCALARS] + [WHOLE] * 8,
        out_specs=[WHOLE] * 7,
        out_shape=[all_fields] + HALO_SHAPES,
        scratch_shapes=[SQUARE] * 4 + y_edges,
        compiler_params=pltpu.CompilerParams(vmem_limit_bytes=12 * MIB),
        name="first_edge",
    )(diffusivity, partial, weights, *halos)
    halos = exchanged(sends)
    partial = pl.pallas_call(
        inner_kernel,
        in_specs=[SCALARS] + [WHOLE] * 3,
        out_specs=WHOLE,
        out_shape=all_fields,
        compiler_params=pltpu.CompilerParams(vmem_limit_bytes=12 * MIB),
        cost_estimate=INNER_COST,
        name="second_inner",
    )(diffusivity, moved, kept, weights)
    sums = [pltpu.VMEM((SPECIES, ROWS, CZ), jnp.float32)] * 4
    out = pl.pallas_call(
        second_edge_kernel,
        in_specs=[SCALARS] * 5 + [WHOLE] * 9,
        out_specs=FAR,
        out_shape=all_fields,
        scratch_shapes=[SQUARE, SQUARE, pltpu.VMEM((FIELDS, ROWS, CZ), jnp.float32), SQUARE]
        + [pltpu.VMEM((SPECIES + 1, ROWS, CZ), jnp.float32)]
        + sums
        + y_edges
        + [
            pltpu.VMEM((8, CZ), jnp.int32),
            pltpu.SMEM((8, CZ), jnp.int32),
            pltpu.SemaphoreType.DMA((3,)),
        ],
        compiler_params=pltpu.CompilerParams(vmem_limit_bytes=20 * MIB),
        name="second_edge",
    )(
        diffusivity, mechanism, prefactor, activation, heat_release,
        partial, weights, work, *halos,
    )
    return out.reshape(FIELDS, CX, CY, CZ)


def solution(mesh):
    grid = P(None, "gx", "gy", "gz")
    placed = (
        grid, grid, grid, P(), P("gx", "gy", "gz"), P("gx", "gy", "gz"), P(), P(), P(), P(),
    )
    return jax.shard_map(body, mesh=mesh, in_specs=placed, out_specs=grid, check_vma=False)
```

```python
import jax
import jax.numpy as jnp
from jax import lax
from jax.experimental import pallas as pl
from jax.experimental.pallas import tpu as pltpu
from jax.sharding import PartitionSpec as P

FIELDS = 40
SPECIES = 22
REACTIONS = 100
SUB = 4
FEW = 80
CX = 8
CY = 16
CZ = 128
ROWS = CX * CY
GROUP = 8
STEPS = FIELDS // GROUP
COURANT = 0.15
CHEM_STEP = 0.25
LOG2E = 1.4426950408889634
AXES = ("gx", "gy", "gz")


def place(axis):
    index = lax.axis_index(axis)
    even = lax.rem(index, 2) == 0
    return even, index > 0, index < lax.axis_size(axis) - 1


def swapped(value, axis, start):
    size = lax.axis_size(axis)
    pairs = []
    for low in range(start, size, 2):
        high = (low + 1) % size
        pairs += [(low, high), (high, low)]
    return lax.ppermute(value, axis, pairs)


def x_rows():
    xeven, _, _ = place("gx")
    high = pl.multiple_of(jnp.where(xeven, (CX - 1) * CY, 0), CY)
    low = pl.multiple_of(jnp.where(xeven, 0, (CX - 1) * CY), CY)
    return high, low


def pick_x(block, sends):
    xs0, xs1 = sends
    high, low = x_rows()
    for f in range(GROUP):
        xs0[f] = block[f, pl.ds(high, CY), :]
        xs1[f] = block[f, pl.ds(low, CY), :]


def pick_yz(step, block, sends, columns):
    ys0, ys1 = sends
    yeven, _, _ = place("gy")
    high_y = jnp.where(yeven, CY - 1, 0)
    low_y = jnp.where(yeven, 0, CY - 1)
    for f in range(GROUP):
        ys0[f] = block[f, pl.ds(high_y, CX, stride=CY), :]
        ys1[f] = block[f, pl.ds(low_y, CX, stride=CY), :]
    lane = lax.broadcasted_iota(jnp.int32, (8, CZ), 1)
    first = step * (2 * GROUP)
    for r in range(0, ROWS, 8):
        total = columns[r : r + 8, :]
        for f in range(GROUP):
            moved = pltpu.roll(block[f, r : r + 8, :], first + 2 * f + 1, 1)
            here = lane - first
            total = jnp.where((here >= 2 * f) & (here < 2 * f + 2), moved, total)
        columns[r : r + 8, :] = total


def turn_faces(zs0, zs1, columns, turned):
    zeven, _, _ = place("gz")
    turned[...] = columns[...].T
    highs = turned[pl.ds(0, FIELDS, stride=2), :]
    lows = turned[pl.ds(1, FIELDS, stride=2), :]
    zs0[...] = jnp.where(zeven, highs, lows)
    zs1[...] = jnp.where(zeven, lows, highs)


def group_of(refs, step):
    return [ref.at[pl.ds(step * GROUP, GROUP)] for ref in refs]


def faces_kernel(
    fields, source, held, kept, xs0, xs1, ys0, ys1, zs0, zs1, columns, turned, sems
):
    def arriving(whole, local, step, k):
        part = pl.ds(step * GROUP, GROUP)
        return pltpu.make_async_copy(whole.at[part], local.at[part], sems.at[k + step])

    for step in range(STEPS):
        arriving(fields, held, step, 0).start()
    for step in range(STEPS):
        arriving(source, kept, step, STEPS).start()
    columns[...] = jnp.zeros_like(columns)

    @pl.loop(0, STEPS)
    def _(step):
        arriving(fields, held, step, 0).wait()
        block, *sends = group_of((held, xs0, xs1, ys0, ys1), step)
        pick_x(block, sends[:2])
        pick_yz(step, block, sends[2:], columns)

    turn_faces(zs0, zs1, columns, turned)
    for step in range(STEPS):
        arriving(source, kept, step, STEPS).wait()


def set_up(velocity, weights):
    for r in range(0, ROWS, 8):
        rest = jnp.ones((8, CZ), jnp.float32)
        for a in range(3):
            speed = velocity[a, r : r + 8, :]
            below = COURANT * jnp.maximum(speed, 0.0)
            above = -COURANT * jnp.minimum(speed, 0.0)
            weights[2 * a, r : r + 8, :] = below
            weights[2 * a + 1, r : r + 8, :] = above
            rest = rest - (below + above)
        weights[6, r : r + 8, :] = rest


def move_group(step, block, source, diffusivity, weights, result):
    row = lax.broadcasted_iota(jnp.int32, (8, CZ), 0)
    lane = lax.broadcasted_iota(jnp.int32, (8, CZ), 1)
    diffuse = [diffusivity[step * GROUP + f] for f in range(GROUP)]
    for low in range(0, ROWS, 8):
        here = slice(low, low + 8)
        before, after = slice(low - 1, low + 7), slice(low + 1, low + 9)
        share = [weights[k, here, :] for k in range(7)]
        size = [share[2 * a] + share[2 * a + 1] for a in range(3)]
        rising = [share[2 * a] > 0.0 for a in range(3)]
        for f in range(GROUP):
            cell = block[f, here, :]
            ym = block[f, before, :] if low > 0 else pltpu.roll(cell, 1, 0)
            yp = block[f, after, :] if low < ROWS - 8 else pltpu.roll(cell, 7, 0)
            if low % CY == 0:
                ym = jnp.where(row == 0, 0.0, ym)
            else:
                yp = jnp.where(row == 7, 0.0, yp)
            zm = jnp.where(lane == 0, 0.0, pltpu.roll(cell, 1, 1))
            zp = jnp.where(lane == CZ - 1, 0.0, pltpu.roll(cell, CZ - 1, 1))
            around = (ym + yp) + (zm + zp)
            carried = size[1] * jnp.where(rising[1], ym, yp)
            carried = carried + size[2] * jnp.where(rising[2], zm, zp)
            if low < CY:
                xp = block[f, low + CY : low + CY + 8, :]
                around, carried = around + xp, carried + share[1] * xp
            elif low >= ROWS - CY:
                xm = block[f, low - CY : low - CY + 8, :]
                around, carried = around + xm, carried + share[0] * xm
            else:
                xm = block[f, low - CY : low - CY + 8, :]
                xp = block[f, low + CY : low + CY + 8, :]
                around = around + (xm + xp)
                carried = carried + size[0] * jnp.where(rising[0], xm, xp)
            kept = cell * (share[6] - 6.0 * diffuse[f])
            result[f, here, :] = (kept + source[f, here, :]) + (carried + diffuse[f] * around)


def turn_halos(zh0, zh1, columns, turned):
    zeven, has_low, has_high = place("gz")
    columns[...] = jnp.zeros_like(columns)
    first, second = zh0[...], zh1[...]
    high = jnp.where(has_high, jnp.where(zeven, first, second), 0.0)
    low = jnp.where(has_low, jnp.where(zeven, second, first), 0.0)
    columns[pl.ds(0, FIELDS, stride=2), :] = high
    columns[pl.ds(1, FIELDS, stride=2), :] = low
    turned[...] = columns[...].T


def close_group(step, partial, halos, diffusivity, weights, turned, y_edges, result):
    xh0, xh1, yh0, yh1 = halos
    y_lows, y_highs = y_edges
    xeven, x_low, x_high = place("gx")
    yeven, y_low, y_high = place("gy")
    row = lax.broadcasted_iota(jnp.int32, (8, CZ), 0)
    lane = lax.broadcasted_iota(jnp.int32, (8, CZ), 1)
    one_low = jnp.where(row == 0, 1.0, 0.0)
    one_high = jnp.where(row == 7, 1.0, 0.0)
    one_z = jnp.where((lane == 0) | (lane == CZ - 1), 1.0, 0.0)
    diffuse = [diffusivity[step * GROUP + f] for f in range(GROUP)]
    for f in range(GROUP):
        first, second = yh0[f], yh1[f]
        y_lows[f] = jnp.where(y_low, jnp.where(yeven, second, first), 0.0)
        y_highs[f] = jnp.where(y_high, jnp.where(yeven, first, second), 0.0)
    for x in range(CX):
        for half in range(2):
            here = slice(x * CY + 8 * half, x * CY + 8 * half + 8)
            part = slice(8 * half, 8 * half + 8)
            edge = turned[here, :]
            share_y = weights[2 + half, here, :] * (one_high if half else one_low)
            share_z = jnp.where(
                lane == 0,
                weights[4, here, :],
                jnp.where(lane == CZ - 1, weights[5, here, :], 0.0),
            )
            for f in range(GROUP):
                y_near = (y_highs if half else y_lows)[f, x : x + 1, :]
                z_near = pltpu.roll(edge, CZ - 1 - 2 * f - step * (2 * GROUP), 1)
                one_y = one_high if half else one_low
                more = (share_y + diffuse[f] * one_y) * y_near
                more = more + (share_z + diffuse[f] * one_z) * z_near
                if x == 0:
                    near = jnp.where(xeven, xh1[f, part, :], xh0[f, part, :])
                    near = jnp.where(x_low, near, 0.0)
                    more = more + (weights[0, here, :] + diffuse[f]) * near
                if x == CX - 1:
                    near = jnp.where(xeven, xh0[f, part, :], xh1[f, part, :])
                    near = jnp.where(x_high, near, 0.0)
                    more = more + (weights[1, here, :] + diffuse[f]) * near
                result[f, here, :] = partial[f, here, :] + more


def first_edge_kernel(
    diffusivity, partial, weights, xh0, xh1, yh0, yh1, zh0, zh1,
    moved, xs0, xs1, ys0, ys1, zs0, zs1, columns, turned, faces, across, y_lows, y_highs,
):
    turn_halos(zh0, zh1, columns, turned)
    faces[...] = jnp.zeros_like(faces)

    @pl.loop(0, STEPS)
    def _(step):
        block, *halos = group_of((partial, xh0, xh1, yh0, yh1), step)
        (result,) = group_of((moved,), step)
        close_group(
            step, block, halos, diffusivity, weights, turned, (y_lows, y_highs), result
        )

    @pl.loop(0, STEPS)
    def _(step):
        result, *sends = group_of((moved, xs0, xs1, ys0, ys1), step)
        pick_x(result, sends[:2])
        pick_yz(step, result, sends[2:], faces)

    turn_faces(zs0, zs1, faces, across)


def first_inner_kernel(diffusivity, fields, source, velocity, partial, weights):
    set_up(velocity, weights)
    inner_kernel(diffusivity, fields, source, weights, partial)


def inner_kernel(diffusivity, fields, source, weights, partial):
    @pl.loop(0, STEPS)
    def _(step):
        block, more, result = group_of((fields, source, partial), step)
        move_group(step, block, more, diffusivity, weights, result)


def rank_blocks(counts, table):
    row = lax.broadcasted_iota(jnp.int32, (ROWS, CZ), 0)
    lane = lax.broadcasted_iota(jnp.int32, (ROWS, CZ), 1)
    mine = counts[...]
    other = mine.T
    ahead = (mine > other) | ((mine == other) & (row < lane))
    ranks = jnp.sum(jnp.where(ahead, 1.0, 0.0), axis=0, keepdims=True)
    down = jnp.broadcast_to(ranks, (ROWS, CZ)).T
    chosen = down == lane.astype(jnp.float32)
    order = jnp.sum(jnp.where(chosen, row.astype(jnp.float32), 0.0), axis=0, keepdims=True)
    longer = jnp.where(mine > lane.astype(jnp.float32), 1.0, 0.0)
    longer = jnp.sum(longer, axis=0, keepdims=True)
    table[0:1, :] = ranks.astype(jnp.int32)
    table[1:2, :] = order.astype(jnp.int32)
    table[2:3, :] = longer.astype(jnp.int32)


def move_rows(count, order, state, ordered, back):
    @pl.loop(0, lax.div(count + 3, 4))
    def _(k):
        for r in range(4):
            place = pl.ds(4 * k + r, 1)
            block = pl.ds(order[1, 4 * k + r], 1)
            for s in range(SPECIES + 1):
                if back:
                    state[s, block, :] = ordered[s, place, :]
                else:
                    ordered[s, place, :] = state[s, block, :]


def react_rows(base, size, unroll, width_of, state, reactions, sums):
    mechanism, prefactor, activation, heat_release = reactions
    taken_a, taken_b, made_c, made_d = sums
    rows = [pl.ds(base + 8 * v, 8) for v in range(size)]
    cold = [1.0 / state[SPECIES, r, :] for r in rows]

    def reaction(j, heats):
        a, b = mechanism[0, j], mechanism[1, j]
        c, d = mechanism[2, j], mechanism[3, j]
        strength, heat = prefactor[j], heat_release[j]
        barrier = -LOG2E * activation[j]
        rates = []
        for v in range(size):
            rate = strength * jnp.exp2(barrier * cold[v])
            rates.append(rate * (state[a, rows[v], :] * state[b, rows[v], :]))
        for part, index in ((taken_a, a), (taken_b, b), (made_c, c), (made_d, d)):
            old = [part[index, rows[v], :] for v in range(size)]
            for v in range(size):
                part[index, rows[v], :] = old[v] + rates[v]
        return tuple(heats[v] + heat * rates[v] for v in range(size))

    nothing = tuple(jnp.zeros((8, CZ), jnp.float32) for _ in range(size))
    heats = lax.fori_loop(0, REACTIONS, reaction, nothing, unroll=unroll)

    widths = []
    for v in range(size):
        width = width_of(rows[v], base + 8 * v)
        widths.append(width)
        state[SPECIES, rows[v], :] = state[SPECIES, rows[v], :] + width * heats[v]

    def species(s, carry):
        empty = jnp.zeros((8, CZ), jnp.float32)
        for v in range(size):
            old = state[s, rows[v], :]
            lost = widths[v] * (taken_a[s, rows[v], :] + taken_b[s, rows[v], :])
            gained = widths[v] * (made_c[s, rows[v], :] + made_d[s, rows[v], :])
            state[s, rows[v], :] = old * ((old + gained) / (old + lost))
        for part in sums:
            for v in range(size):
                part[s, rows[v], :] = empty
        return carry

    lax.fori_loop(0, SPECIES, species, 0)

def react_sorted(first, state, order, reactions, sums):
    @pl.loop(first, SUB)
    def _(number):
        def width_of(rows, low):
            place = lax.broadcasted_iota(jnp.int32, (8, CZ), 0) + low
            many = jnp.ones((8, CZ), jnp.float32)
            for k in range(1, SUB):
                many = many + jnp.where(place < order[2, k], 1.0, 0.0)
            return jnp.where(place < order[2, number], CHEM_STEP / many, 0.0)

        active = order[2, number]

        @pl.when(active > 40)
        def _():
            react_rows(0, 10, 4, width_of, state, reactions, sums)

        @pl.when((active > 0) & (active <= 40))
        def _():
            react_rows(0, 5, 5, width_of, state, reactions, sums)


def react_all(last, state, counts, reactions, sums):
    @pl.loop(0, last)
    def _(number):
        def width_of(rows, low):
            many = counts[rows, :]
            live = many > number.astype(jnp.float32)
            return jnp.where(live, CHEM_STEP / jnp.maximum(many, 1.0), 0.0)

        react_rows(0, ROWS // 8, 4, width_of, state, reactions, sums)


def second_edge_kernel(
    diffusivity, mechanism, prefactor, activation, heat_release,
    partial, weights, work, xh0, xh1, yh0, yh1, zh0, zh1,
    out, columns, turned, state, counts, ordered, sum_a, sum_b, sum_c, sum_d, y_lows, y_highs,
    table, order, sems,
):
    def leaving(low, many, k):
        part = pl.ds(low, many)
        return pltpu.make_async_copy(state.at[part], out.at[part], sems.at[k])

    columns[...] = jnp.zeros_like(columns)
    columns[0:CX, 0:CY] = work[...]
    turned[...] = columns[...].T
    for x in range(CX):
        counts[x * CY : (x + 1) * CY, :] = jnp.broadcast_to(turned[0:CY, x : x + 1], (CY, CZ))
    rank_blocks(counts, table)
    listing = pltpu.make_async_copy(table, order, sems.at[0])
    listing.start()
    turn_halos(zh0, zh1, columns, turned)

    @pl.loop(0, STEPS)
    def _(step):
        block, *halos = group_of((partial, xh0, xh1, yh0, yh1), step)
        (result,) = group_of((state,), step)
        for part in (sum_a, sum_b, sum_c, sum_d):
            for k in range(5):
                s = jnp.minimum(5 * step + k, SPECIES - 1)
                part[s] = jnp.zeros((ROWS, CZ), jnp.float32)
        close_group(
            step, block, halos, diffusivity, weights, turned, (y_lows, y_highs), result
        )

    listing.wait()
    rest = leaving(SPECIES + 1, FIELDS - SPECIES - 1, 1)
    rest.start()

    reactions = (mechanism, prefactor, activation, heat_release)
    sums = (sum_a, sum_b, sum_c, sum_d)
    full = jnp.int32(0)
    for k in range(SUB):
        full = full + jnp.where(order[2, k] > FEW, 1, 0)
    react_all(full, state, counts, reactions, sums)

    @pl.when(full < SUB)
    def _():
        moving = order[2, full]
        move_rows(moving, order, state, ordered, False)
        react_sorted(full, ordered, order, reactions, sums)
        move_rows(moving, order, state, ordered, True)

    leaving(0, SPECIES + 1, 2).start()
    rest.wait()
    leaving(0, SPECIES + 1, 2).wait()


SCALARS = pl.BlockSpec(memory_space=pltpu.SMEM)
WHOLE = pl.BlockSpec(memory_space=pltpu.VMEM)
FAR = pl.BlockSpec(memory_space=pltpu.HBM)
HALO_SHAPES = [
    jax.ShapeDtypeStruct(shape, jnp.float32)
    for shape in (
        (FIELDS, CY, CZ), (FIELDS, CY, CZ), (FIELDS, CX, CZ), (FIELDS, CX, CZ),
        (FIELDS, CZ), (FIELDS, CZ),
    )
]
SQUARE = pltpu.VMEM((ROWS, CZ), jnp.float32)
MIB = 1024 * 1024
FACES_LIMIT = 47 * MIB
INNER_COST = pl.CostEstimate(flops=60_000_000, bytes_accessed=8_000_000, transcendentals=0)


def exchanged_along(k, sends):
    return [swapped(sends[0], AXES[k], 0), swapped(sends[1], AXES[k], 1)]


def exchanged(sends):
    return [half for k in range(3) for half in exchanged_along(k, sends[2 * k : 2 * k + 2])]


def body(
    fields, source, velocity, diffusivity, reacting, counts, mechanism, prefactor, activation,
    heat_release,
):
    fields = fields.reshape(FIELDS, ROWS, CZ)
    source = source.reshape(FIELDS, ROWS, CZ)
    velocity = velocity.reshape(3, ROWS, CZ)
    work = jnp.where(reacting == 1, counts, 0).astype(jnp.float32).reshape(CX, CY)
    all_fields = jax.ShapeDtypeStruct((FIELDS, ROWS, CZ), jnp.float32)
    all_weights = jax.ShapeDtypeStruct((7, ROWS, CZ), jnp.float32)
    y_edges = [pltpu.VMEM((GROUP, CX, CZ), jnp.float32)] * 2

    held, kept, *sends = pl.pallas_call(
        faces_kernel,
        in_specs=[FAR] * 2,
        out_specs=[WHOLE] * 8,
        out_shape=[all_fields, all_fields] + HALO_SHAPES,
        scratch_shapes=[SQUARE, SQUARE, pltpu.SemaphoreType.DMA((2 * STEPS,))],
        compiler_params=pltpu.CompilerParams(vmem_limit_bytes=FACES_LIMIT),
        name="faces",
    )(fields, source)
    halos = exchanged(sends)
    partial, weights = pl.pallas_call(
        first_inner_kernel,
        in_specs=[SCALARS] + [WHOLE] * 3,
        out_specs=[WHOLE] * 2,
        out_shape=[all_fields, all_weights],
        compiler_params=pltpu.CompilerParams(vmem_limit_bytes=12 * MIB),
        cost_estimate=INNER_COST,
        name="first_inner",
    )(diffusivity, held, kept, velocity)
    moved, *sends = pl.pallas_call(
        first_edge_kernel,
        in_specs=[SCALARS] + [WHOLE] * 8,
        out_specs=[WHOLE] * 7,
        out_shape=[all_fields] + HALO_SHAPES,
        scratch_shapes=[SQUARE] * 4 + y_edges,
        compiler_params=pltpu.CompilerParams(vmem_limit_bytes=12 * MIB),
        name="first_edge",
    )(diffusivity, partial, weights, *halos)
    halos = exchanged(sends)
    partial = pl.pallas_call(
        inner_kernel,
        in_specs=[SCALARS] + [WHOLE] * 3,
        out_specs=WHOLE,
        out_shape=all_fields,
        compiler_params=pltpu.CompilerParams(vmem_limit_bytes=12 * MIB),
        cost_estimate=INNER_COST,
        name="second_inner",
    )(diffusivity, moved, kept, weights)
    sums = [pltpu.VMEM((SPECIES, ROWS, CZ), jnp.float32)] * 4
    out = pl.pallas_call(
        second_edge_kernel,
        in_specs=[SCALARS] * 5 + [WHOLE] * 9,
        out_specs=FAR,
        out_shape=all_fields,
        scratch_shapes=[SQUARE, SQUARE, pltpu.VMEM((FIELDS, ROWS, CZ), jnp.float32), SQUARE]
        + [pltpu.VMEM((SPECIES + 1, ROWS, CZ), jnp.float32)]
        + sums
        + y_edges
        + [
            pltpu.VMEM((8, CZ), jnp.int32),
            pltpu.SMEM((8, CZ), jnp.int32),
            pltpu.SemaphoreType.DMA((3,)),
        ],
        compiler_params=pltpu.CompilerParams(vmem_limit_bytes=20 * MIB),
        name="second_edge",
    )(
        diffusivity, mechanism, prefactor, activation, heat_release,
        partial, weights, work, *halos,
    )
    return out.reshape(FIELDS, CX, CY, CZ)


def solution(mesh):
    grid = P(None, "gx", "gy", "gz")
    placed = (
        grid, grid, grid, P(), P("gx", "gy", "gz"), P("gx", "gy", "gz"), P(), P(), P(), P(),
    )
    return jax.shard_map(body, mesh=mesh, in_specs=placed, out_specs=grid, check_vma=False)
```

```python
import jax
import jax.numpy as jnp
from jax import lax
from jax.experimental import pallas as pl
from jax.experimental.pallas import tpu as pltpu
from jax.sharding import PartitionSpec as P

FIELDS = 40
SPECIES = 22
REACTIONS = 100
SUB = 4
FEW = 80
CX = 8
CY = 16
CZ = 128
ROWS = CX * CY
GROUP = 8
STEPS = FIELDS // GROUP
COURANT = 0.15
CHEM_STEP = 0.25
LOG2E = 1.4426950408889634
AXES = ("gx", "gy", "gz")


def place(axis):
    index = lax.axis_index(axis)
    even = lax.rem(index, 2) == 0
    return even, index > 0, index < lax.axis_size(axis) - 1


def swapped(value, axis, start):
    size = lax.axis_size(axis)
    pairs = []
    for low in range(start, size, 2):
        high = (low + 1) % size
        pairs += [(low, high), (high, low)]
    return lax.ppermute(value, axis, pairs)


def x_rows():
    xeven, _, _ = place("gx")
    high = pl.multiple_of(jnp.where(xeven, (CX - 1) * CY, 0), CY)
    low = pl.multiple_of(jnp.where(xeven, 0, (CX - 1) * CY), CY)
    return high, low


def pick_x(block, sends):
    xs0, xs1 = sends
    high, low = x_rows()
    for f in range(GROUP):
        xs0[f] = block[f, pl.ds(high, CY), :]
        xs1[f] = block[f, pl.ds(low, CY), :]


def pick_yz(step, block, sends, columns):
    ys0, ys1 = sends
    yeven, _, _ = place("gy")
    high_y = jnp.where(yeven, CY - 1, 0)
    low_y = jnp.where(yeven, 0, CY - 1)
    for f in range(GROUP):
        ys0[f] = block[f, pl.ds(high_y, CX, stride=CY), :]
        ys1[f] = block[f, pl.ds(low_y, CX, stride=CY), :]
    lane = lax.broadcasted_iota(jnp.int32, (8, CZ), 1)
    first = step * (2 * GROUP)
    for r in range(0, ROWS, 8):
        total = columns[r : r + 8, :]
        for f in range(GROUP):
            moved = pltpu.roll(block[f, r : r + 8, :], first + 2 * f + 1, 1)
            here = lane - first
            total = jnp.where((here >= 2 * f) & (here < 2 * f + 2), moved, total)
        columns[r : r + 8, :] = total


def turn_faces(zs0, zs1, columns, turned):
    zeven, _, _ = place("gz")
    turned[...] = columns[...].T
    highs = turned[pl.ds(0, FIELDS, stride=2), :]
    lows = turned[pl.ds(1, FIELDS, stride=2), :]
    zs0[...] = jnp.where(zeven, highs, lows)
    zs1[...] = jnp.where(zeven, lows, highs)


def group_of(refs, step):
    return [ref.at[pl.ds(step * GROUP, GROUP)] for ref in refs]


def faces_kernel(
    fields, source, held, kept, xs0, xs1, ys0, ys1, zs0, zs1, columns, turned, sems
):
    def arriving(whole, local, step, k):
        part = pl.ds(step * GROUP, GROUP)
        return pltpu.make_async_copy(whole.at[part], local.at[part], sems.at[k + step])

    for step in range(STEPS):
        arriving(fields, held, step, 0).start()
    for step in range(STEPS):
        arriving(source, kept, step, STEPS).start()
    columns[...] = jnp.zeros_like(columns)

    @pl.loop(0, STEPS)
    def _(step):
        arriving(fields, held, step, 0).wait()
        block, *sends = group_of((held, xs0, xs1, ys0, ys1), step)
        pick_x(block, sends[:2])
        pick_yz(step, block, sends[2:], columns)

    turn_faces(zs0, zs1, columns, turned)
    for step in range(STEPS):
        arriving(source, kept, step, STEPS).wait()


def set_up(velocity, weights):
    for r in range(0, ROWS, 8):
        rest = jnp.ones((8, CZ), jnp.float32)
        for a in range(3):
            speed = velocity[a, r : r + 8, :]
            below = COURANT * jnp.maximum(speed, 0.0)
            above = -COURANT * jnp.minimum(speed, 0.0)
            weights[2 * a, r : r + 8, :] = below
            weights[2 * a + 1, r : r + 8, :] = above
            rest = rest - (below + above)
        weights[6, r : r + 8, :] = rest


def move_group(block, source, diffusivity, weights, result):
    row = lax.broadcasted_iota(jnp.int32, (8, CZ), 0)
    lane = lax.broadcasted_iota(jnp.int32, (8, CZ), 1)
    diffuse = [jnp.broadcast_to(diffusivity[f : f + 1, :], (8, CZ)) for f in range(GROUP)]
    for low in range(0, ROWS, 8):
        here = slice(low, low + 8)
        before, after = slice(low - 1, low + 7), slice(low + 1, low + 9)
        share = [weights[k, here, :] for k in range(7)]
        size = [share[2 * a] + share[2 * a + 1] for a in range(3)]
        rising = [share[2 * a] > 0.0 for a in range(3)]
        for f in range(GROUP):
            cell = block[f, here, :]
            ym = block[f, before, :] if low > 0 else pltpu.roll(cell, 1, 0)
            yp = block[f, after, :] if low < ROWS - 8 else pltpu.roll(cell, 7, 0)
            if low % CY == 0:
                ym = jnp.where(row == 0, 0.0, ym)
            else:
                yp = jnp.where(row == 7, 0.0, yp)
            zm = jnp.where(lane == 0, 0.0, pltpu.roll(cell, 1, 1))
            zp = jnp.where(lane == CZ - 1, 0.0, pltpu.roll(cell, CZ - 1, 1))
            around = (ym + yp) + (zm + zp)
            carried = size[1] * jnp.where(rising[1], ym, yp)
            carried = carried + size[2] * jnp.where(rising[2], zm, zp)
            if low < CY:
                xp = block[f, low + CY : low + CY + 8, :]
                around, carried = around + xp, carried + share[1] * xp
            elif low >= ROWS - CY:
                xm = block[f, low - CY : low - CY + 8, :]
                around, carried = around + xm, carried + share[0] * xm
            else:
                xm = block[f, low - CY : low - CY + 8, :]
                xp = block[f, low + CY : low + CY + 8, :]
                around = around + (xm + xp)
                carried = carried + size[0] * jnp.where(rising[0], xm, xp)
            kept = cell * (share[6] - 6.0 * diffuse[f])
            result[f, here, :] = (kept + source[f, here, :]) + (carried + diffuse[f] * around)


def turn_halos(zh0, zh1, columns, turned):
    zeven, has_low, has_high = place("gz")
    columns[...] = jnp.zeros_like(columns)
    first, second = zh0[...], zh1[...]
    high = jnp.where(has_high, jnp.where(zeven, first, second), 0.0)
    low = jnp.where(has_low, jnp.where(zeven, second, first), 0.0)
    columns[pl.ds(0, FIELDS, stride=2), :] = high
    columns[pl.ds(1, FIELDS, stride=2), :] = low
    turned[...] = columns[...].T


def close_group(step, partial, halos, diffusivity, weights, turned, y_edges, result):
    xh0, xh1, yh0, yh1 = halos
    y_lows, y_highs = y_edges
    xeven, x_low, x_high = place("gx")
    yeven, y_low, y_high = place("gy")
    row = lax.broadcasted_iota(jnp.int32, (8, CZ), 0)
    lane = lax.broadcasted_iota(jnp.int32, (8, CZ), 1)
    one_low = jnp.where(row == 0, 1.0, 0.0)
    one_high = jnp.where(row == 7, 1.0, 0.0)
    one_z = jnp.where((lane == 0) | (lane == CZ - 1), 1.0, 0.0)
    diffuse = [jnp.broadcast_to(diffusivity[f : f + 1, :], (8, CZ)) for f in range(GROUP)]
    for f in range(GROUP):
        first, second = yh0[f], yh1[f]
        y_lows[f] = jnp.where(y_low, jnp.where(yeven, second, first), 0.0)
        y_highs[f] = jnp.where(y_high, jnp.where(yeven, first, second), 0.0)
    for x in range(CX):
        for half in range(2):
            here = slice(x * CY + 8 * half, x * CY + 8 * half + 8)
            part = slice(8 * half, 8 * half + 8)
            edge = turned[here, :]
            share_y = weights[2 + half, here, :] * (one_high if half else one_low)
            share_z = jnp.where(
                lane == 0,
                weights[4, here, :],
                jnp.where(lane == CZ - 1, weights[5, here, :], 0.0),
            )
            for f in range(GROUP):
                y_near = (y_highs if half else y_lows)[f, x : x + 1, :]
                z_near = pltpu.roll(edge, CZ - 1 - 2 * f - step * (2 * GROUP), 1)
                one_y = one_high if half else one_low
                more = (share_y + diffuse[f] * one_y) * y_near
                more = more + (share_z + diffuse[f] * one_z) * z_near
                if x == 0:
                    near = jnp.where(xeven, xh1[f, part, :], xh0[f, part, :])
                    near = jnp.where(x_low, near, 0.0)
                    more = more + (weights[0, here, :] + diffuse[f]) * near
                if x == CX - 1:
                    near = jnp.where(xeven, xh0[f, part, :], xh1[f, part, :])
                    near = jnp.where(x_high, near, 0.0)
                    more = more + (weights[1, here, :] + diffuse[f]) * near
                result[f, here, :] = partial[f, here, :] + more


def first_edge_kernel(
    diffusivity, partial, weights, xh0, xh1, yh0, yh1, zh0, zh1,
    moved, xs0, xs1, ys0, ys1, zs0, zs1, columns, turned, faces, across, y_lows, y_highs,
):
    turn_halos(zh0, zh1, columns, turned)
    faces[...] = jnp.zeros_like(faces)

    @pl.loop(0, STEPS)
    def _(step):
        block, *halos = group_of((partial, xh0, xh1, yh0, yh1), step)
        spread, result = group_of((diffusivity, moved), step)
        close_group(
            step, block, halos, spread, weights, turned, (y_lows, y_highs), result
        )

    @pl.loop(0, STEPS)
    def _(step):
        result, *sends = group_of((moved, xs0, xs1, ys0, ys1), step)
        pick_x(result, sends[:2])
        pick_yz(step, result, sends[2:], faces)

    turn_faces(zs0, zs1, faces, across)


def first_inner_kernel(
    diffusivity, fields, source, velocity, partial, weights, spread, columns, turned
):
    columns[...] = jnp.zeros_like(columns)
    columns[:, 0:FIELDS] = jnp.broadcast_to(diffusivity[...], (ROWS, FIELDS))
    turned[...] = columns[...].T
    spread[...] = turned[0:FIELDS, :]
    set_up(velocity, weights)
    inner_kernel(spread, fields, source, weights, partial)


def inner_kernel(diffusivity, fields, source, weights, partial):
    @pl.loop(0, STEPS)
    def _(step):
        block, more, spread, result = group_of((fields, source, diffusivity, partial), step)
        move_group(block, more, spread, weights, result)


def rank_blocks(counts, table):
    row = lax.broadcasted_iota(jnp.int32, (ROWS, CZ), 0)
    lane = lax.broadcasted_iota(jnp.int32, (ROWS, CZ), 1)
    mine = counts[...]
    other = mine.T
    ahead = (mine > other) | ((mine == other) & (row < lane))
    ranks = jnp.sum(jnp.where(ahead, 1.0, 0.0), axis=0, keepdims=True)
    down = jnp.broadcast_to(ranks, (ROWS, CZ)).T
    chosen = down == lane.astype(jnp.float32)
    order = jnp.sum(jnp.where(chosen, row.astype(jnp.float32), 0.0), axis=0, keepdims=True)
    longer = jnp.where(mine > lane.astype(jnp.float32), 1.0, 0.0)
    longer = jnp.sum(longer, axis=0, keepdims=True)
    table[0:1, :] = ranks.astype(jnp.int32)
    table[1:2, :] = order.astype(jnp.int32)
    table[2:3, :] = longer.astype(jnp.int32)


def move_rows(count, order, state, ordered, back):
    @pl.loop(0, lax.div(count + 3, 4))
    def _(k):
        for r in range(4):
            place = pl.ds(4 * k + r, 1)
            block = pl.ds(order[1, 4 * k + r], 1)
            for s in range(SPECIES + 1):
                if back:
                    state[s, block, :] = ordered[s, place, :]
                else:
                    ordered[s, place, :] = state[s, block, :]


def react_rows(base, size, unroll, width_of, state, reactions, sums):
    mechanism, prefactor, activation, heat_release = reactions
    taken_a, taken_b, made_c, made_d = sums
    rows = [pl.ds(base + 8 * v, 8) for v in range(size)]
    cold = [1.0 / state[SPECIES, r, :] for r in rows]

    def reaction(j, heats):
        a, b = mechanism[0, j], mechanism[1, j]
        c, d = mechanism[2, j], mechanism[3, j]
        strength, heat = prefactor[j], heat_release[j]
        barrier = -LOG2E * activation[j]
        rates = []
        for v in range(size):
            rate = strength * jnp.exp2(barrier * cold[v])
            rates.append(rate * (state[a, rows[v], :] * state[b, rows[v], :]))
        for part, index in ((taken_a, a), (taken_b, b), (made_c, c), (made_d, d)):
            old = [part[index, rows[v], :] for v in range(size)]
            for v in range(size):
                part[index, rows[v], :] = old[v] + rates[v]
        return tuple(heats[v] + heat * rates[v] for v in range(size))

    nothing = tuple(jnp.zeros((8, CZ), jnp.float32) for _ in range(size))
    heats = lax.fori_loop(0, REACTIONS, reaction, nothing, unroll=unroll)

    widths = []
    for v in range(size):
        width = width_of(rows[v], base + 8 * v)
        widths.append(width)
        state[SPECIES, rows[v], :] = state[SPECIES, rows[v], :] + width * heats[v]

    def species(s, carry):
        empty = jnp.zeros((8, CZ), jnp.float32)
        for v in range(size):
            old = state[s, rows[v], :]
            lost = widths[v] * (taken_a[s, rows[v], :] + taken_b[s, rows[v], :])
            gained = widths[v] * (made_c[s, rows[v], :] + made_d[s, rows[v], :])
            state[s, rows[v], :] = old * ((old + gained) / (old + lost))
        for part in sums:
            for v in range(size):
                part[s, rows[v], :] = empty
        return carry

    lax.fori_loop(0, SPECIES, species, 0)

def react_sorted(first, state, order, reactions, sums):
    @pl.loop(first, SUB)
    def _(number):
        def width_of(rows, low):
            place = lax.broadcasted_iota(jnp.int32, (8, CZ), 0) + low
            many = jnp.ones((8, CZ), jnp.float32)
            for k in range(1, SUB):
                many = many + jnp.where(place < order[2, k], 1.0, 0.0)
            return jnp.where(place < order[2, number], CHEM_STEP / many, 0.0)

        active = order[2, number]

        @pl.when(active > 40)
        def _():
            react_rows(0, 10, 4, width_of, state, reactions, sums)

        @pl.when((active > 0) & (active <= 40))
        def _():
            react_rows(0, 5, 5, width_of, state, reactions, sums)


def react_all(last, state, counts, reactions, sums):
    @pl.loop(0, last)
    def _(number):
        def width_of(rows, low):
            many = counts[rows, :]
            live = many > number.astype(jnp.float32)
            return jnp.where(live, CHEM_STEP / jnp.maximum(many, 1.0), 0.0)

        react_rows(0, ROWS // 8, 4, width_of, state, reactions, sums)


def second_edge_kernel(
    diffusivity, far_mechanism, far_prefactor, far_activation, far_heat_release,
    partial, weights, work, xh0, xh1, yh0, yh1, zh0, zh1,
    out, columns, turned, state, counts, ordered, sum_a, sum_b, sum_c, sum_d, y_lows, y_highs,
    table, order, mechanism, prefactor, activation, heat_release, sems,
):
    far = (far_mechanism, far_prefactor, far_activation, far_heat_release)
    near = (mechanism, prefactor, activation, heat_release)
    reading = [
        pltpu.make_async_copy(there, here, sems.at[3 + k])
        for k, (there, here) in enumerate(zip(far, near))
    ]
    for copy in reading:
        copy.start()

    def leaving(low, many, k):
        part = pl.ds(low, many)
        return pltpu.make_async_copy(state.at[part], out.at[part], sems.at[k])

    columns[...] = jnp.zeros_like(columns)
    columns[0:CX, 0:CY] = work[...]
    turned[...] = columns[...].T
    for x in range(CX):
        counts[x * CY : (x + 1) * CY, :] = jnp.broadcast_to(turned[0:CY, x : x + 1], (CY, CZ))
    rank_blocks(counts, table)
    listing = pltpu.make_async_copy(table, order, sems.at[0])
    listing.start()
    turn_halos(zh0, zh1, columns, turned)

    @pl.loop(0, STEPS)
    def _(step):
        block, *halos = group_of((partial, xh0, xh1, yh0, yh1), step)
        spread, result = group_of((diffusivity, state), step)
        for part in (sum_a, sum_b, sum_c, sum_d):
            for k in range(5):
                s = jnp.minimum(5 * step + k, SPECIES - 1)
                part[s] = jnp.zeros((ROWS, CZ), jnp.float32)
        close_group(
            step, block, halos, spread, weights, turned, (y_lows, y_highs), result
        )

    listing.wait()
    for copy in reading:
        copy.wait()
    rest = leaving(SPECIES + 1, FIELDS - SPECIES - 1, 1)
    rest.start()

    reactions = (mechanism, prefactor, activation, heat_release)
    sums = (sum_a, sum_b, sum_c, sum_d)
    full = jnp.int32(0)
    for k in range(SUB):
        full = full + jnp.where(order[2, k] > FEW, 1, 0)
    react_all(full, state, counts, reactions, sums)

    @pl.when(full < SUB)
    def _():
        moving = order[2, full]
        move_rows(moving, order, state, ordered, False)
        react_sorted(full, ordered, order, reactions, sums)
        move_rows(moving, order, state, ordered, True)

    leaving(0, SPECIES + 1, 2).start()
    rest.wait()
    leaving(0, SPECIES + 1, 2).wait()


WHOLE = pl.BlockSpec(memory_space=pltpu.VMEM)
FAR = pl.BlockSpec(memory_space=pltpu.HBM)
HALO_SHAPES = [
    jax.ShapeDtypeStruct(shape, jnp.float32)
    for shape in (
        (FIELDS, CY, CZ), (FIELDS, CY, CZ), (FIELDS, CX, CZ), (FIELDS, CX, CZ),
        (FIELDS, CZ), (FIELDS, CZ),
    )
]
SQUARE = pltpu.VMEM((ROWS, CZ), jnp.float32)
MIB = 1024 * 1024
FACES_LIMIT = 47 * MIB
INNER_COST = pl.CostEstimate(flops=60_000_000, bytes_accessed=8_000_000, transcendentals=0)


def exchanged_along(k, sends):
    return [swapped(sends[0], AXES[k], 0), swapped(sends[1], AXES[k], 1)]


def exchanged(sends):
    return [half for k in range(3) for half in exchanged_along(k, sends[2 * k : 2 * k + 2])]


def body(
    fields, source, velocity, diffusivity, reacting, counts, mechanism, prefactor, activation,
    heat_release,
):
    fields = fields.reshape(FIELDS, ROWS, CZ)
    source = source.reshape(FIELDS, ROWS, CZ)
    velocity = velocity.reshape(3, ROWS, CZ)
    work = jnp.where(reacting == 1, counts, 0).astype(jnp.float32).reshape(CX, CY)
    all_fields = jax.ShapeDtypeStruct((FIELDS, ROWS, CZ), jnp.float32)
    all_weights = jax.ShapeDtypeStruct((7, ROWS, CZ), jnp.float32)
    y_edges = [pltpu.VMEM((GROUP, CX, CZ), jnp.float32)] * 2

    held, kept, *sends = pl.pallas_call(
        faces_kernel,
        in_specs=[FAR] * 2,
        out_specs=[WHOLE] * 8,
        out_shape=[all_fields, all_fields] + HALO_SHAPES,
        scratch_shapes=[SQUARE, SQUARE, pltpu.SemaphoreType.DMA((2 * STEPS,))],
        compiler_params=pltpu.CompilerParams(vmem_limit_bytes=FACES_LIMIT),
        name="faces",
    )(fields, source)
    halos = exchanged(sends)
    partial, weights, spread = pl.pallas_call(
        first_inner_kernel,
        in_specs=[WHOLE] * 4,
        out_specs=[WHOLE] * 3,
        out_shape=[all_fields, all_weights, HALO_SHAPES[-1]],
        scratch_shapes=[SQUARE, SQUARE],
        compiler_params=pltpu.CompilerParams(vmem_limit_bytes=12 * MIB),
        cost_estimate=INNER_COST,
        name="first_inner",
    )(diffusivity.reshape(1, FIELDS), held, kept, velocity)
    moved, *sends = pl.pallas_call(
        first_edge_kernel,
        in_specs=[WHOLE] * 9,
        out_specs=[WHOLE] * 7,
        out_shape=[all_fields] + HALO_SHAPES,
        scratch_shapes=[SQUARE] * 4 + y_edges,
        compiler_params=pltpu.CompilerParams(vmem_limit_bytes=12 * MIB),
        name="first_edge",
    )(spread, partial, weights, *halos)
    halos = exchanged(sends)
    partial = pl.pallas_call(
        inner_kernel,
        in_specs=[WHOLE] * 4,
        out_specs=WHOLE,
        out_shape=all_fields,
        compiler_params=pltpu.CompilerParams(vmem_limit_bytes=12 * MIB),
        cost_estimate=INNER_COST,
        name="second_inner",
    )(spread, moved, kept, weights)
    sums = [pltpu.VMEM((SPECIES, ROWS, CZ), jnp.float32)] * 4
    out = pl.pallas_call(
        second_edge_kernel,
        in_specs=[WHOLE] + [FAR] * 4 + [WHOLE] * 9,
        out_specs=FAR,
        out_shape=all_fields,
        scratch_shapes=[SQUARE, SQUARE, pltpu.VMEM((FIELDS, ROWS, CZ), jnp.float32), SQUARE]
        + [pltpu.VMEM((SPECIES + 1, ROWS, CZ), jnp.float32)]
        + sums
        + y_edges
        + [
            pltpu.VMEM((8, CZ), jnp.int32),
            pltpu.SMEM((8, CZ), jnp.int32),
            pltpu.SMEM((4, REACTIONS), jnp.int32),
            pltpu.SMEM((REACTIONS,), jnp.float32),
            pltpu.SMEM((REACTIONS,), jnp.float32),
            pltpu.SMEM((REACTIONS,), jnp.float32),
            pltpu.SemaphoreType.DMA((7,)),
        ],
        compiler_params=pltpu.CompilerParams(vmem_limit_bytes=20 * MIB),
        name="second_edge",
    )(
        spread, mechanism, prefactor, activation, heat_release,
        partial, weights, work, *halos,
    )
    return out.reshape(FIELDS, CX, CY, CZ)


def solution(mesh):
    grid = P(None, "gx", "gy", "gz")
    placed = (
        grid, grid, grid, P(), P("gx", "gy", "gz"), P("gx", "gy", "gz"), P(), P(), P(), P(),
    )
    return jax.shard_map(body, mesh=mesh, in_specs=placed, out_specs=grid, check_vma=False)
```

```python
import jax
import jax.numpy as jnp
from jax import lax
from jax.experimental import pallas as pl
from jax.experimental.pallas import tpu as pltpu
from jax.sharding import PartitionSpec as P

FIELDS = 40
SPECIES = 22
REACTIONS = 100
SUB = 4
FEW = 80
CX = 8
CY = 16
CZ = 128
ROWS = CX * CY
GROUP = 8
STEPS = FIELDS // GROUP
COURANT = 0.15
CHEM_STEP = 0.25
LOG2E = 1.4426950408889634
AXES = ("gx", "gy", "gz")


def place(axis):
    index = lax.axis_index(axis)
    even = lax.rem(index, 2) == 0
    return even, index > 0, index < lax.axis_size(axis) - 1


def swapped(value, axis, start):
    size = lax.axis_size(axis)
    pairs = []
    for low in range(start, size, 2):
        high = (low + 1) % size
        pairs += [(low, high), (high, low)]
    return lax.ppermute(value, axis, pairs)


def x_rows():
    xeven, _, _ = place("gx")
    high = pl.multiple_of(jnp.where(xeven, (CX - 1) * CY, 0), CY)
    low = pl.multiple_of(jnp.where(xeven, 0, (CX - 1) * CY), CY)
    return high, low


def pick_x(block, sends):
    xs0, xs1 = sends
    high, low = x_rows()
    for f in range(GROUP):
        xs0[f] = block[f, pl.ds(high, CY), :]
        xs1[f] = block[f, pl.ds(low, CY), :]


def pick_yz(step, block, sends, columns):
    ys0, ys1 = sends
    yeven, _, _ = place("gy")
    high_y = jnp.where(yeven, CY - 1, 0)
    low_y = jnp.where(yeven, 0, CY - 1)
    for f in range(GROUP):
        ys0[f] = block[f, pl.ds(high_y, CX, stride=CY), :]
        ys1[f] = block[f, pl.ds(low_y, CX, stride=CY), :]
    lane = lax.broadcasted_iota(jnp.int32, (8, CZ), 1)
    first = step * (2 * GROUP)
    for r in range(0, ROWS, 8):
        total = columns[r : r + 8, :]
        for f in range(GROUP):
            moved = pltpu.roll(block[f, r : r + 8, :], first + 2 * f + 1, 1)
            here = lane - first
            total = jnp.where((here >= 2 * f) & (here < 2 * f + 2), moved, total)
        columns[r : r + 8, :] = total


def turn_faces(zs0, zs1, columns, turned):
    zeven, _, _ = place("gz")
    turned[...] = columns[...].T
    highs = turned[pl.ds(0, FIELDS, stride=2), :]
    lows = turned[pl.ds(1, FIELDS, stride=2), :]
    zs0[...] = jnp.where(zeven, highs, lows)
    zs1[...] = jnp.where(zeven, lows, highs)


def group_of(refs, step):
    return [ref.at[pl.ds(step * GROUP, GROUP)] for ref in refs]


def faces_kernel(
    fields, source, held, kept, xs0, xs1, ys0, ys1, zs0, zs1, columns, turned, sems
):
    def arriving(whole, local, step, k):
        part = pl.ds(step * GROUP, GROUP)
        return pltpu.make_async_copy(whole.at[part], local.at[part], sems.at[k + step])

    for step in range(STEPS):
        arriving(fields, held, step, 0).start()
    for step in range(STEPS):
        arriving(source, kept, step, STEPS).start()
    columns[...] = jnp.zeros_like(columns)

    @pl.loop(0, STEPS)
    def _(step):
        arriving(fields, held, step, 0).wait()
        block, *sends = group_of((held, xs0, xs1, ys0, ys1), step)
        pick_x(block, sends[:2])
        pick_yz(step, block, sends[2:], columns)

    turn_faces(zs0, zs1, columns, turned)
    for step in range(STEPS):
        arriving(source, kept, step, STEPS).wait()


def set_up(velocity, weights):
    for r in range(0, ROWS, 8):
        rest = jnp.ones((8, CZ), jnp.float32)
        for a in range(3):
            speed = velocity[a, r : r + 8, :]
            below = COURANT * jnp.maximum(speed, 0.0)
            above = -COURANT * jnp.minimum(speed, 0.0)
            weights[2 * a, r : r + 8, :] = below
            weights[2 * a + 1, r : r + 8, :] = above
            rest = rest - (below + above)
        weights[6, r : r + 8, :] = rest


def move_group(block, source, diffusivity, weights, result):
    row = lax.broadcasted_iota(jnp.int32, (8, CZ), 0)
    lane = lax.broadcasted_iota(jnp.int32, (8, CZ), 1)
    diffuse = [jnp.broadcast_to(diffusivity[f : f + 1, :], (8, CZ)) for f in range(GROUP)]
    for low in range(0, ROWS, 8):
        here = slice(low, low + 8)
        before, after = slice(low - 1, low + 7), slice(low + 1, low + 9)
        share = [weights[k, here, :] for k in range(7)]
        size = [share[2 * a] + share[2 * a + 1] for a in range(3)]
        rising = [share[2 * a] > 0.0 for a in range(3)]
        for f in range(GROUP):
            cell = block[f, here, :]
            ym = block[f, before, :] if low > 0 else pltpu.roll(cell, 1, 0)
            yp = block[f, after, :] if low < ROWS - 8 else pltpu.roll(cell, 7, 0)
            if low % CY == 0:
                ym = jnp.where(row == 0, 0.0, ym)
            else:
                yp = jnp.where(row == 7, 0.0, yp)
            zm = jnp.where(lane == 0, 0.0, pltpu.roll(cell, 1, 1))
            zp = jnp.where(lane == CZ - 1, 0.0, pltpu.roll(cell, CZ - 1, 1))
            around = (ym + yp) + (zm + zp)
            carried = size[1] * jnp.where(rising[1], ym, yp)
            carried = carried + size[2] * jnp.where(rising[2], zm, zp)
            if low < CY:
                xp = block[f, low + CY : low + CY + 8, :]
                around, carried = around + xp, carried + share[1] * xp
            elif low >= ROWS - CY:
                xm = block[f, low - CY : low - CY + 8, :]
                around, carried = around + xm, carried + share[0] * xm
            else:
                xm = block[f, low - CY : low - CY + 8, :]
                xp = block[f, low + CY : low + CY + 8, :]
                around = around + (xm + xp)
                carried = carried + size[0] * jnp.where(rising[0], xm, xp)
            kept = cell * (share[6] - 6.0 * diffuse[f])
            result[f, here, :] = (kept + source[f, here, :]) + (carried + diffuse[f] * around)


def turn_halos(zh0, zh1, columns, turned):
    zeven, has_low, has_high = place("gz")
    columns[...] = jnp.zeros_like(columns)
    first, second = zh0[...], zh1[...]
    high = jnp.where(has_high, jnp.where(zeven, first, second), 0.0)
    low = jnp.where(has_low, jnp.where(zeven, second, first), 0.0)
    columns[pl.ds(0, FIELDS, stride=2), :] = high
    columns[pl.ds(1, FIELDS, stride=2), :] = low
    turned[...] = columns[...].T


def close_group(step, partial, halos, diffusivity, weights, turned, y_edges, result):
    xh0, xh1, yh0, yh1 = halos
    y_lows, y_highs = y_edges
    xeven, x_low, x_high = place("gx")
    yeven, y_low, y_high = place("gy")
    row = lax.broadcasted_iota(jnp.int32, (8, CZ), 0)
    lane = lax.broadcasted_iota(jnp.int32, (8, CZ), 1)
    one_low = jnp.where(row == 0, 1.0, 0.0)
    one_high = jnp.where(row == 7, 1.0, 0.0)
    one_z = jnp.where((lane == 0) | (lane == CZ - 1), 1.0, 0.0)
    diffuse = [jnp.broadcast_to(diffusivity[f : f + 1, :], (8, CZ)) for f in range(GROUP)]
    for f in range(GROUP):
        first, second = yh0[f], yh1[f]
        y_lows[f] = jnp.where(y_low, jnp.where(yeven, second, first), 0.0)
        y_highs[f] = jnp.where(y_high, jnp.where(yeven, first, second), 0.0)
    for x in range(CX):
        for half in range(2):
            here = slice(x * CY + 8 * half, x * CY + 8 * half + 8)
            part = slice(8 * half, 8 * half + 8)
            edge = turned[here, :]
            share_y = weights[2 + half, here, :] * (one_high if half else one_low)
            share_z = jnp.where(
                lane == 0,
                weights[4, here, :],
                jnp.where(lane == CZ - 1, weights[5, here, :], 0.0),
            )
            for f in range(GROUP):
                y_near = (y_highs if half else y_lows)[f, x : x + 1, :]
                z_near = pltpu.roll(edge, CZ - 1 - 2 * f - step * (2 * GROUP), 1)
                one_y = one_high if half else one_low
                more = (share_y + diffuse[f] * one_y) * y_near
                more = more + (share_z + diffuse[f] * one_z) * z_near
                if x == 0:
                    near = jnp.where(xeven, xh1[f, part, :], xh0[f, part, :])
                    near = jnp.where(x_low, near, 0.0)
                    more = more + (weights[0, here, :] + diffuse[f]) * near
                if x == CX - 1:
                    near = jnp.where(xeven, xh0[f, part, :], xh1[f, part, :])
                    near = jnp.where(x_high, near, 0.0)
                    more = more + (weights[1, here, :] + diffuse[f]) * near
                result[f, here, :] = partial[f, here, :] + more


def first_edge_kernel(
    diffusivity, partial, weights, xh0, xh1, yh0, yh1, zh0, zh1,
    moved, xs0, xs1, ys0, ys1, zs0, zs1, columns, turned, faces, across, y_lows, y_highs,
):
    turn_halos(zh0, zh1, columns, turned)
    faces[...] = jnp.zeros_like(faces)

    @pl.loop(0, STEPS)
    def _(step):
        block, *halos = group_of((partial, xh0, xh1, yh0, yh1), step)
        spread, result = group_of((diffusivity, moved), step)
        close_group(
            step, block, halos, spread, weights, turned, (y_lows, y_highs), result
        )

    @pl.loop(0, STEPS)
    def _(step):
        result, *sends = group_of((moved, xs0, xs1, ys0, ys1), step)
        pick_x(result, sends[:2])
        pick_yz(step, result, sends[2:], faces)

    turn_faces(zs0, zs1, faces, across)


def first_inner_kernel(
    diffusivity, fields, source, velocity, partial, weights, spread, columns, turned
):
    columns[...] = jnp.zeros_like(columns)
    columns[:, 0:FIELDS] = jnp.broadcast_to(diffusivity[...], (ROWS, FIELDS))
    turned[...] = columns[...].T
    spread[...] = turned[0:FIELDS, :]
    set_up(velocity, weights)
    inner_kernel(spread, fields, source, weights, partial)


def inner_kernel(diffusivity, fields, source, weights, partial):
    @pl.loop(0, STEPS)
    def _(step):
        block, more, spread, result = group_of((fields, source, diffusivity, partial), step)
        move_group(block, more, spread, weights, result)


def rank_blocks(counts, table):
    row = lax.broadcasted_iota(jnp.int32, (ROWS, CZ), 0)
    lane = lax.broadcasted_iota(jnp.int32, (ROWS, CZ), 1)
    mine = counts[...]
    other = mine.T
    ahead = (mine > other) | ((mine == other) & (row < lane))
    ranks = jnp.sum(jnp.where(ahead, 1.0, 0.0), axis=0, keepdims=True)
    down = jnp.broadcast_to(ranks, (ROWS, CZ)).T
    chosen = down == lane.astype(jnp.float32)
    order = jnp.sum(jnp.where(chosen, row.astype(jnp.float32), 0.0), axis=0, keepdims=True)
    longer = jnp.where(mine > lane.astype(jnp.float32), 1.0, 0.0)
    longer = jnp.sum(longer, axis=0, keepdims=True)
    table[0:1, :] = ranks.astype(jnp.int32)
    table[1:2, :] = order.astype(jnp.int32)
    table[2:3, :] = longer.astype(jnp.int32)


def move_rows(count, order, state, ordered, back):
    @pl.loop(0, lax.div(count + 3, 4))
    def _(k):
        for r in range(4):
            place = pl.ds(4 * k + r, 1)
            block = pl.ds(order[1, 4 * k + r], 1)
            for s in range(SPECIES + 1):
                if back:
                    state[s, block, :] = ordered[s, place, :]
                else:
                    ordered[s, place, :] = state[s, block, :]


def react_rows(base, size, unroll, width_of, state, reactions, sums):
    mechanism, prefactor, activation, heat_release = reactions
    taken_a, taken_b, made_c, made_d = sums
    rows = [pl.ds(base + 8 * v, 8) for v in range(size)]
    cold = [1.0 / state[SPECIES, r, :] for r in rows]

    def reaction(j, heats):
        a, b = mechanism[0, j], mechanism[1, j]
        c, d = mechanism[2, j], mechanism[3, j]
        strength, heat = prefactor[j], heat_release[j]
        barrier = -LOG2E * activation[j]
        rates = []
        for v in range(size):
            rate = strength * jnp.exp2(barrier * cold[v])
            rates.append(rate * (state[a, rows[v], :] * state[b, rows[v], :]))
        for part, index in ((taken_a, a), (taken_b, b), (made_c, c), (made_d, d)):
            old = [part[index, rows[v], :] for v in range(size)]
            for v in range(size):
                part[index, rows[v], :] = old[v] + rates[v]
        return tuple(heats[v] + heat * rates[v] for v in range(size))

    nothing = tuple(jnp.zeros((8, CZ), jnp.float32) for _ in range(size))
    heats = lax.fori_loop(0, REACTIONS, reaction, nothing, unroll=unroll)

    widths = []
    for v in range(size):
        width = width_of(rows[v], base + 8 * v)
        widths.append(width)
        state[SPECIES, rows[v], :] = state[SPECIES, rows[v], :] + width * heats[v]

    def species(s, carry):
        empty = jnp.zeros((8, CZ), jnp.float32)
        for v in range(size):
            old = state[s, rows[v], :]
            lost = widths[v] * (taken_a[s, rows[v], :] + taken_b[s, rows[v], :])
            gained = widths[v] * (made_c[s, rows[v], :] + made_d[s, rows[v], :])
            state[s, rows[v], :] = old * ((old + gained) / (old + lost))
        for part in sums:
            for v in range(size):
                part[s, rows[v], :] = empty
        return carry

    lax.fori_loop(0, SPECIES, species, 0)

def react_sorted(first, state, order, reactions, sums):
    @pl.loop(first, SUB)
    def _(number):
        def width_of(rows, low):
            place = lax.broadcasted_iota(jnp.int32, (8, CZ), 0) + low
            many = jnp.ones((8, CZ), jnp.float32)
            for k in range(1, SUB):
                many = many + jnp.where(place < order[2, k], 1.0, 0.0)
            return jnp.where(place < order[2, number], CHEM_STEP / many, 0.0)

        active = order[2, number]

        @pl.when(active > 40)
        def _():
            react_rows(0, 10, 5, width_of, state, reactions, sums)

        @pl.when((active > 0) & (active <= 40))
        def _():
            react_rows(0, 5, 10, width_of, state, reactions, sums)


def react_all(last, state, counts, reactions, sums):
    @pl.loop(0, last)
    def _(number):
        def width_of(rows, low):
            many = counts[rows, :]
            live = many > number.astype(jnp.float32)
            return jnp.where(live, CHEM_STEP / jnp.maximum(many, 1.0), 0.0)

        react_rows(0, ROWS // 8, 4, width_of, state, reactions, sums)


def second_edge_kernel(
    diffusivity, far_mechanism, far_prefactor, far_activation, far_heat_release,
    partial, weights, work, xh0, xh1, yh0, yh1, zh0, zh1,
    out, columns, turned, state, counts, ordered, sum_a, sum_b, sum_c, sum_d, y_lows, y_highs,
    table, order, mechanism, prefactor, activation, heat_release, sems,
):
    far = (far_mechanism, far_prefactor, far_activation, far_heat_release)
    near = (mechanism, prefactor, activation, heat_release)
    reading = [
        pltpu.make_async_copy(there, here, sems.at[3 + k])
        for k, (there, here) in enumerate(zip(far, near))
    ]
    for copy in reading:
        copy.start()

    def leaving(low, many, k):
        part = pl.ds(low, many)
        return pltpu.make_async_copy(state.at[part], out.at[part], sems.at[k])

    columns[...] = jnp.zeros_like(columns)
    columns[0:CX, 0:CY] = work[...]
    turned[...] = columns[...].T
    for x in range(CX):
        counts[x * CY : (x + 1) * CY, :] = jnp.broadcast_to(turned[0:CY, x : x + 1], (CY, CZ))
    rank_blocks(counts, table)
    listing = pltpu.make_async_copy(table, order, sems.at[0])
    listing.start()
    turn_halos(zh0, zh1, columns, turned)

    @pl.loop(0, STEPS)
    def _(step):
        block, *halos = group_of((partial, xh0, xh1, yh0, yh1), step)
        spread, result = group_of((diffusivity, state), step)
        for part in (sum_a, sum_b, sum_c, sum_d):
            for k in range(5):
                s = jnp.minimum(5 * step + k, SPECIES - 1)
                part[s] = jnp.zeros((ROWS, CZ), jnp.float32)
        close_group(
            step, block, halos, spread, weights, turned, (y_lows, y_highs), result
        )

    listing.wait()
    for copy in reading:
        copy.wait()
    rest = leaving(SPECIES + 1, FIELDS - SPECIES - 1, 1)
    rest.start()

    reactions = (mechanism, prefactor, activation, heat_release)
    sums = (sum_a, sum_b, sum_c, sum_d)
    full = jnp.int32(0)
    for k in range(SUB):
        full = full + jnp.where(order[2, k] > FEW, 1, 0)
    react_all(full, state, counts, reactions, sums)

    @pl.when(full < SUB)
    def _():
        moving = order[2, full]
        move_rows(moving, order, state, ordered, False)
        react_sorted(full, ordered, order, reactions, sums)
        move_rows(moving, order, state, ordered, True)

    leaving(0, SPECIES + 1, 2).start()
    rest.wait()
    leaving(0, SPECIES + 1, 2).wait()


WHOLE = pl.BlockSpec(memory_space=pltpu.VMEM)
FAR = pl.BlockSpec(memory_space=pltpu.HBM)
HALO_SHAPES = [
    jax.ShapeDtypeStruct(shape, jnp.float32)
    for shape in (
        (FIELDS, CY, CZ), (FIELDS, CY, CZ), (FIELDS, CX, CZ), (FIELDS, CX, CZ),
        (FIELDS, CZ), (FIELDS, CZ),
    )
]
SQUARE = pltpu.VMEM((ROWS, CZ), jnp.float32)
MIB = 1024 * 1024
FACES_LIMIT = 47 * MIB
INNER_COST = pl.CostEstimate(flops=60_000_000, bytes_accessed=8_000_000, transcendentals=0)


def exchanged_along(k, sends):
    return [swapped(sends[0], AXES[k], 0), swapped(sends[1], AXES[k], 1)]


def exchanged(sends):
    return [half for k in range(3) for half in exchanged_along(k, sends[2 * k : 2 * k + 2])]


def body(
    fields, source, velocity, diffusivity, reacting, counts, mechanism, prefactor, activation,
    heat_release,
):
    fields = fields.reshape(FIELDS, ROWS, CZ)
    source = source.reshape(FIELDS, ROWS, CZ)
    velocity = velocity.reshape(3, ROWS, CZ)
    work = jnp.where(reacting == 1, counts, 0).astype(jnp.float32).reshape(CX, CY)
    all_fields = jax.ShapeDtypeStruct((FIELDS, ROWS, CZ), jnp.float32)
    all_weights = jax.ShapeDtypeStruct((7, ROWS, CZ), jnp.float32)
    y_edges = [pltpu.VMEM((GROUP, CX, CZ), jnp.float32)] * 2

    held, kept, *sends = pl.pallas_call(
        faces_kernel,
        in_specs=[FAR] * 2,
        out_specs=[WHOLE] * 8,
        out_shape=[all_fields, all_fields] + HALO_SHAPES,
        scratch_shapes=[SQUARE, SQUARE, pltpu.SemaphoreType.DMA((2 * STEPS,))],
        compiler_params=pltpu.CompilerParams(vmem_limit_bytes=FACES_LIMIT),
        name="faces",
    )(fields, source)
    halos = exchanged(sends)
    partial, weights, spread = pl.pallas_call(
        first_inner_kernel,
        in_specs=[WHOLE] * 4,
        out_specs=[WHOLE] * 3,
        out_shape=[all_fields, all_weights, HALO_SHAPES[-1]],
        scratch_shapes=[SQUARE, SQUARE],
        compiler_params=pltpu.CompilerParams(vmem_limit_bytes=12 * MIB),
        cost_estimate=INNER_COST,
        name="first_inner",
    )(diffusivity.reshape(1, FIELDS), held, kept, velocity)
    moved, *sends = pl.pallas_call(
        first_edge_kernel,
        in_specs=[WHOLE] * 9,
        out_specs=[WHOLE] * 7,
        out_shape=[all_fields] + HALO_SHAPES,
        scratch_shapes=[SQUARE] * 4 + y_edges,
        compiler_params=pltpu.CompilerParams(vmem_limit_bytes=12 * MIB),
        name="first_edge",
    )(spread, partial, weights, *halos)
    halos = exchanged(sends)
    partial = pl.pallas_call(
        inner_kernel,
        in_specs=[WHOLE] * 4,
        out_specs=WHOLE,
        out_shape=all_fields,
        compiler_params=pltpu.CompilerParams(vmem_limit_bytes=12 * MIB),
        cost_estimate=INNER_COST,
        name="second_inner",
    )(spread, moved, kept, weights)
    sums = [pltpu.VMEM((SPECIES, ROWS, CZ), jnp.float32)] * 4
    out = pl.pallas_call(
        second_edge_kernel,
        in_specs=[WHOLE] + [FAR] * 4 + [WHOLE] * 9,
        out_specs=FAR,
        out_shape=all_fields,
        scratch_shapes=[SQUARE, SQUARE, pltpu.VMEM((FIELDS, ROWS, CZ), jnp.float32), SQUARE]
        + [pltpu.VMEM((SPECIES + 1, ROWS, CZ), jnp.float32)]
        + sums
        + y_edges
        + [
            pltpu.VMEM((8, CZ), jnp.int32),
            pltpu.SMEM((8, CZ), jnp.int32),
            pltpu.SMEM((4, REACTIONS), jnp.int32),
            pltpu.SMEM((REACTIONS,), jnp.float32),
            pltpu.SMEM((REACTIONS,), jnp.float32),
            pltpu.SMEM((REACTIONS,), jnp.float32),
            pltpu.SemaphoreType.DMA((7,)),
        ],
        compiler_params=pltpu.CompilerParams(vmem_limit_bytes=20 * MIB),
        name="second_edge",
    )(
        spread, mechanism, prefactor, activation, heat_release,
        partial, weights, work, *halos,
    )
    return out.reshape(FIELDS, CX, CY, CZ)


def solution(mesh):
    grid = P(None, "gx", "gy", "gz")
    placed = (
        grid, grid, grid, P(), P("gx", "gy", "gz"), P("gx", "gy", "gz"), P(), P(), P(), P(),
    )
    return jax.shard_map(body, mesh=mesh, in_specs=placed, out_specs=grid, check_vma=False)
```
